256 devices in a mesh: rows: 128 (over z, y_lo, x, core), dp: 2 (over y_hi).
Axes of the slice: x: 4, y: 4 (y_hi: 2, y_lo: 2; y = y_hi * 2 + y_lo), z: 8, core: 2. Of those that a mesh axis runs over, the one named last changes fastest.
Arguments:
- query_act: bfloat16 [1024, 512, 128], P(('dp', 'rows')), parts along dimension 0, may hold values from -2.09375 to 2.09375
- key_act: bfloat16 [1024, 512, 128], P(('dp', 'rows')), parts along dimension 0, may hold values from -2.09375 to 2.09375
- value_act: bfloat16 [1024, 512, 128], P(('dp', 'rows')), parts along dimension 0, may hold values from -4 to 4
- attn_out: bfloat16 [1024, 512, 128], P(('dp', 'rows')), parts along dimension 0, may hold values from -4 to 4
- grad_out: bfloat16 [1024, 512, 128], P(('dp', 'rows')), parts along dimension 0, may hold values from -24 to 24
- pair_bias: bfloat16 [4, 1024, 512], P(None, ('dp', 'rows')), parts along dimension 1, may hold values from -3 to 3
- log_norm: float32 [1024, 4, 512], P(('dp', 'rows')), parts along dimension 0, may hold values from 6.8 to 8
- back_weight: bfloat16 [384, 128], replicated, may hold values from -2 to 2
Outputs:
- column_grad: bfloat16 [512, 1024, 128], P('rows', 'dp'), parts along dimension 1
- bias_grad: float32 [4, 1024, 512], P(None, ('dp', 'rows')), parts along dimension 1
The draws below stay inside these ranges and needn't reach their ends.
There are 2 independent parts, one for each index of `dp`. The reference program is written for one: setup_inputs(seed, part) draws one part's arguments, and reference() takes and returns one part's arrays. A program takes and returns all parts, laid end to end along the dimension named above; an argument that names none is the same for every part. Nothing has to cross between parts.
All inputs are finite; a program needn't handle non-finite values.
Results may differ from the reference program's by a relative error of at most 0.008.
Values may be sent and summed in bfloat16 or wider, within the bound.
No kernel may reach another device: no remote copies, remote signals or barrier semaphores. Data moves between devices by JAX's collectives and lax.ppermute only.
A program may use at most 64 MiB of HBM per device.

```python
import jax
import jax.numpy as jnp
from jax import lax

C = 128
HEADS = 4
HD = 128
N = 512


def raised(array, own_key, source, target, parts, factor):
    def block_of(position):
        return (jnp.arange(array.shape[position]) // (array.shape[position] // parts)).reshape((-1,) + (1,) * (array.ndim - 1 - position))

    first = jax.random.permutation(own_key, parts)[block_of(target)]
    far = (block_of(target) + parts // 2) % parts
    return jnp.where((block_of(source) == first) | (block_of(source) == far), factor * array, array)


def block_levels(own_key, dims, cuts, low, high):
    def one(axis_at, shards_of):
        steps = jax.random.uniform(jax.random.fold_in(jax.random.fold_in(own_key, 6), axis_at), (shards_of,), jnp.float32, low / len(cuts), high / len(cuts))
        return jnp.repeat(jnp.exp(steps), dims[axis_at] // shards_of).reshape((-1,) + (1,) * (len(dims) - axis_at - 1))

    loudness = one(*cuts[0])
    for cut in cuts[1:]:
        loudness = loudness * one(*cut)
    return loudness


def scatter_about(key, dims, width, most, cuts=(), dtype=jnp.bfloat16):
    level = block_levels(key, dims, cuts, -0.22, 0.18) if cuts else 1.0
    result = jax.random.normal(key, dims, jnp.float32) * width * level
    return jnp.minimum(jnp.maximum(result, -most), most).astype(dtype)


def heavy_noise(stream_key, dims, spread, most, cuts, heavy, kind=jnp.bfloat16):
    drawn = spread * jax.random.normal(stream_key, dims, jnp.float32)
    if cuts:
        drawn = drawn * block_levels(stream_key, dims, cuts, -0.22, 0.18)
    return jnp.clip(raised(drawn, jax.random.fold_in(stream_key, 3), *heavy), -most, most).astype(kind)


def setup_inputs(seed: int = 0, part: int = 0) -> dict:
    seeds = jax.random.split(jax.random.key(seed), 9)
    own_keys = jax.random.split(jax.random.fold_in(seeds[8], part), 9)
    query_act = scatter_about(own_keys[0], (N, N, HD), 0.7, 2.09375, ((0, 128),))
    key_act = scatter_about(own_keys[1], (N, N, HD), 0.7, 2.09375, ((0, 128),))
    value_act = scatter_about(own_keys[2], (N, N, HD), 1.0, 4.0, ((0, 128),))
    attn_out = scatter_about(own_keys[3], (N, N, HD), 1.0, 4.0, ((0, 128),))
    grad_out = heavy_noise(own_keys[4], (N, N, HD), 1.0, 24.0, ((0, 128),), (0, 1, 128, 5.5))
    pair_bias = scatter_about(own_keys[5], (HEADS, N, N), 1.0, 3.0, ((1, 128),))
    log_norm = jnp.clip(6.8 + 1.1999998 * jax.random.uniform(own_keys[6], (N, HEADS, N), jnp.float32) ** block_levels(own_keys[6], (N, HEADS, N), ((0, 128),), -0.2, 0.2), 6.8, 8.0)
    back_weight = scatter_about(seeds[7], (3 * HD, C), 0.5, 2.0)
    return {"query_act": query_act, "key_act": key_act, "value_act": value_act, "attn_out": attn_out, "grad_out": grad_out, "pair_bias": pair_bias, "log_norm": log_norm, "back_weight": back_weight}


def reference(query_act, key_act, value_act, attn_out, grad_out, pair_bias, log_norm, back_weight):
    length = query_act.shape[1]
    head_count = pair_bias.shape[0]
    head_size = query_act.shape[2] // head_count
    softmax_scale = head_size ** -0.5
    bias_full = pair_bias.astype(jnp.float32)

    def single_row(running, inputs):
        query_row, key_row, value_row, out_row, grad_row, norm_row = inputs
        query_h = query_row.astype(jnp.float32).reshape(length, head_count, head_size)
        key_h = key_row.astype(jnp.float32).reshape(length, head_count, head_size)
        value_h = value_row.astype(jnp.float32).reshape(length, head_count, head_size)
        out_h = out_row.astype(jnp.float32).reshape(length, head_count, head_size)
        grad_h = grad_row.astype(jnp.float32).reshape(length, head_count, head_size)
        scores = jnp.einsum("jhd,khd->hjk", query_h, key_h) * softmax_scale + bias_full
        probs = jnp.exp(scores - norm_row[:, :, None])
        probs_low = lax.optimization_barrier(probs.astype(jnp.bfloat16)).astype(jnp.float32)
        grad_value = jnp.einsum("hjk,jhd->khd", probs_low, grad_h)
        grad_prob = jnp.einsum("jhd,khd->hjk", grad_h, value_h)
        row_delta = jnp.einsum("jhd,jhd->hj", grad_h, out_h)
        grad_score = probs * (grad_prob - row_delta[:, :, None])
        score_low = lax.optimization_barrier(grad_score.astype(jnp.bfloat16)).astype(jnp.float32)
        grad_query = jnp.einsum("hjk,khd->jhd", score_low, key_h) * softmax_scale
        grad_key = jnp.einsum("hjk,jhd->khd", score_low, query_h) * softmax_scale
        joined = jnp.concatenate([grad_query.reshape(length, -1), grad_key.reshape(length, -1), grad_value.reshape(length, -1)], axis=1).astype(jnp.bfloat16)
        pair_row = jnp.dot(joined, back_weight, preferred_element_type=jnp.float32).astype(jnp.bfloat16)
        return running + grad_score, pair_row

    initial = jnp.zeros(pair_bias.shape, jnp.float32)
    bias_grad, pair_rows = lax.scan(single_row, initial, (query_act, key_act, value_act, attn_out, grad_out, log_norm))
    return jnp.transpose(pair_rows, (1, 0, 2)), bias_grad
```

```python
import functools

import jax
import jax.numpy as jnp
from jax import lax
from jax.experimental import pallas as pl
from jax.experimental.pallas import tpu as pltpu
from jax.sharding import Mesh
from jax.sharding import PartitionSpec as P

Z, Y, X, C = ("rows_0", "rows_1", "rows_2", "rows_3")
ROWS = (Z, Y, X, C)
DP_ROWS = ("dp",) + ROWS
PLANE = (Y, X)
LINE = (Z, C)
LOG2E = 1.4426950408889634


def exchange(x, axes):
    return lax.all_to_all(x, axes, split_axis=0, concat_axis=0, tiled=True)


def across(x):
    return lax.ppermute(x, C, [(0, 1), (1, 0)])


def attention_rows(
    first, core_ref, q_ref, k_ref, v_ref, o_ref, g_ref, ln_ref, bias_ref, w_ref, *rest
):
    if first:
        pair_ref, db_ref, b2, kvt, qt, gt = rest
    else:
        before_ref, pair_ref, wire_ref, b2, kvt, qt, gt, db_ref = rest
    step = pl.program_id(0)
    planes, heads, lines, tall, length = bias_ref.shape
    width = q_ref.shape[2]
    size = 32
    scale = size**-0.5
    core = core_ref[0]

    @pl.when(step == 0)
    def _():
        for h in range(heads):
            for a in range(planes):
                for z in range(lines):
                    at = (z * planes + a) * tall
                    b2[h, at : at + tall, :] = bias_ref[a, h, z].astype(jnp.float32) * LOG2E
        if first:
            db_ref[...] = jnp.zeros_like(db_ref)
        else:
            db_ref[...] = before_ref[...]

    q, k, v, g = q_ref[0], k_ref[0], v_ref[0], g_ref[0]
    qt[...] = q.T
    gt[...] = g.T
    kt = k.T
    vt = v.T
    product = g.astype(jnp.float32) * o_ref[0].astype(jnp.float32)
    lane = lax.broadcasted_iota(jnp.int32, (1, width), 1)
    ln_lane = lax.broadcasted_iota(jnp.int32, (1, ln_ref.shape[2]), 1)
    block = 256
    grad_q = [None] * (length // block)
    for h in range(heads):
        head = core * heads + h
        mine = (lane // size) == head
        ln = jnp.sum(jnp.where(ln_lane == head, ln_ref[0], 0.0), axis=1, keepdims=True) * LOG2E
        delta = jnp.sum(jnp.where(mine, product, 0.0), axis=1, keepdims=True)
        zero = jnp.zeros_like(q)
        qh = jnp.where(mine, q, zero)
        gh = jnp.where(mine, g, zero)
        kh = jnp.where(mine, k, zero)
        rows = pl.ds(pl.multiple_of(head * size, size), size)
        qth = qt[rows, :]
        gth = gt[rows, :]
        grad_k = None
        for b in range(length // block):
            span = slice(b * block, (b + 1) * block)
            s = jnp.dot(qh[span], kt, preferred_element_type=jnp.float32)
            d = jnp.dot(gh[span], vt, preferred_element_type=jnp.float32)
            p = jnp.exp2(s * (scale * LOG2E) + b2[h, span, :] - ln[span])
            ds = p * (d - delta[span])
            db_ref[h, span, :] += ds
            pb = p.astype(jnp.bfloat16)
            dsb = ds.astype(jnp.bfloat16)
            gv = jnp.dot(gth[:, span], pb, preferred_element_type=jnp.float32)
            gk = jnp.dot(qth[:, span], dsb, preferred_element_type=jnp.float32)
            gq = jnp.dot(dsb, kh, preferred_element_type=jnp.float32)
            grad_k = gk if grad_k is None else grad_k + gk
            grad_v = gv if b == 0 else grad_v + gv
            grad_q[b] = gq if grad_q[b] is None else grad_q[b] + gq
        kvt[h * size : (h + 1) * size, :] = (grad_k * scale).astype(jnp.bfloat16)
        kvt[(heads + h) * size : (heads + h + 1) * size, :] = grad_v.astype(jnp.bfloat16)
    half = heads * size
    own = pl.multiple_of(core * half, half)
    w_kv = jnp.concatenate(
        [w_ref[pl.ds(width + own, half), :], w_ref[pl.ds(2 * width + own, half), :]], axis=0
    )
    kv = kvt[...].T
    for b in range(length // block):
        span = slice(b * block, (b + 1) * block)
        total = jnp.dot(
            (grad_q[b] * scale).astype(jnp.bfloat16), w_ref[:width, :], preferred_element_type=jnp.float32
        ) + jnp.dot(kv[span], w_kv, preferred_element_type=jnp.float32)
        pair_ref[0, span, :] = total.astype(pair_ref.dtype)

    if not first:

        @pl.when(step == pl.num_programs(0) - 1)
        def _():
            for h in range(heads):
                for a in range(planes):
                    for z in range(lines):
                        at = (z * planes + a) * tall
                        wire_ref[a, h, z] = db_ref[h, at : at + tall, :].astype(wire_ref.dtype)


def run_rows(core, acts, bias, weight, before=None):
    first = before is None
    rows, length, width = acts[0].shape
    heads = bias.shape[1]
    row = pl.BlockSpec((1, length, width), lambda i: (i, 0, 0))
    whole = lambda x: pl.BlockSpec(x.shape, lambda i: (0,) * len(x.shape))
    ln = acts[-1]
    in_specs = [pl.BlockSpec(memory_space=pltpu.SMEM)] + [row] * 5
    in_specs += [pl.BlockSpec((1,) + ln.shape[1:], lambda i: (i, 0, 0)), whole(bias), whole(weight)]
    args = [core, *acts, bias, weight]
    square = jax.ShapeDtypeStruct((heads, length, length), jnp.float32)
    scratch = [
        pltpu.VMEM(square.shape, jnp.float32),
        pltpu.VMEM((width, length), jnp.bfloat16),
        pltpu.VMEM((width, length), jnp.bfloat16),
        pltpu.VMEM((width, length), jnp.bfloat16),
    ]
    if first:
        outs = [jax.ShapeDtypeStruct((rows, length, width), jnp.bfloat16), square]
        out_specs = [row, whole(square)]
    else:
        args.append(before)
        in_specs.append(whole(before))
        outs = [
            jax.ShapeDtypeStruct((rows, length, width), jnp.float32),
            jax.ShapeDtypeStruct(bias.shape, jnp.bfloat16),
        ]
        out_specs = [row, whole(bias)]
        scratch.append(pltpu.VMEM(square.shape, jnp.float32))
    return pl.pallas_call(
        functools.partial(attention_rows, first),
        grid=(rows,),
        in_specs=in_specs,
        out_specs=out_specs,
        out_shape=outs,
        scratch_shapes=scratch,
        compiler_params=pltpu.CompilerParams(dimension_semantics=("arbitrary",)),
        cost_estimate=pl.CostEstimate(
            flops=10 * rows * heads * length * length * width,
            bytes_accessed=8 * 1024 * 1024,
            transcendentals=rows * heads * length * length,
        ),
        name="partner_rows" if first else "own_rows",
    )(*args)


def local(query_act, key_act, value_act, attn_out, grad_out, pair_bias, log_norm, back_weight):
    heads, tall, length = pair_bias.shape
    z_n, c_n = lax.axis_size(Z), lax.axis_size(C)
    p_n = lax.axis_size(Y) * lax.axis_size(X)
    near = heads // c_n
    core = lax.axis_index(C).astype(jnp.int32).reshape(1)

    tiles = jnp.broadcast_to(
        pair_bias.reshape(1, c_n, near * tall, length), (z_n, c_n, near * tall, length)
    )
    lines = exchange(tiles.reshape(z_n * c_n, near * tall, length), LINE)
    lines = lines.reshape(z_n, c_n, near, tall, length).transpose(2, 0, 1, 3, 4)
    lines = lines.reshape(1, near * z_n * c_n * tall, length)
    planes = exchange(jnp.broadcast_to(lines, (p_n, *lines.shape[1:])), PLANE)
    bias = planes.reshape(p_n, near, z_n, c_n * tall, length)

    own = (query_act, key_act, value_act, attn_out, grad_out, jnp.swapaxes(log_norm, 1, 2))
    other = tuple(across(x) for x in own[:5]) + (jnp.swapaxes(across(log_norm), 1, 2),)

    sent, half_sum = run_rows(core, other, bias, back_weight)
    kept, terms = run_rows(core, own, bias, back_weight, half_sum)
    pair_rows = (kept + across(sent).astype(jnp.float32)).astype(jnp.bfloat16)

    summed = exchange(terms.reshape(p_n, -1, length), PLANE).astype(jnp.float32).sum(axis=0)
    summed = summed.reshape(near, z_n, c_n, tall, length).transpose(1, 2, 0, 3, 4)
    summed = summed.astype(jnp.bfloat16).reshape(z_n * c_n, near * tall, length)
    summed = exchange(summed, LINE).reshape(z_n, heads, tall, length)
    bias_grad = summed.astype(jnp.float32).sum(axis=0)

    swapped = jnp.transpose(pair_rows, (1, 0, 2))
    column_grad = lax.all_to_all(swapped, ROWS, split_axis=0, concat_axis=1, tiled=True)
    return (column_grad, bias_grad)


def solution(mesh):
    finer = Mesh(mesh.devices.reshape(8, 2, 4, 2, mesh.shape["dp"]), (*ROWS, "dp"))
    row = P(DP_ROWS, None, None)
    return jax.shard_map(
        local,
        mesh=finer,
        in_specs=(row, row, row, row, row, P(None, DP_ROWS, None), row, P()),
        out_specs=(P(ROWS, "dp", None), P(None, DP_ROWS, None)),
        check_vma=False,
    )
```

```python
import functools

import jax
import jax.numpy as jnp
from jax import lax
from jax.experimental import pallas as pl
from jax.experimental.pallas import tpu as pltpu
from jax.sharding import Mesh
from jax.sharding import PartitionSpec as P

Z, Y, X, C = ("rows_0", "rows_1", "rows_2", "rows_3")
ROWS = (Z, Y, X, C)
DP_ROWS = ("dp",) + ROWS
LOG2E = 1.4426950408889634


def swapped_with(x, axes, mask):
    n = lax.axis_size(axes)
    return lax.ppermute(x, axes, [(i, i ^ mask) for i in range(n)])


def across(x):
    return swapped_with(x, C, 1)


def attention_rows(
    first, planes, place_ref, q_ref, k_ref, v_ref, o_ref, g_ref, ln_ref, w_ref, *rest
):
    bias_refs, rest = rest[:planes], rest[planes:]
    if first:
        pair_ref, db_ref, b2, kvt, qt, gt = rest
    else:
        before_ref, pair_ref, *wire_refs, b2, kvt, qt, gt, db_ref = rest
    step = pl.program_id(0)
    lines, heads, tall, length = bias_refs[0].shape
    width = q_ref.shape[2]
    size = 32
    scale = size**-0.5
    core = place_ref[0]

    def placed(a, z):
        at = ((place_ref[1] ^ z) * planes + (place_ref[2] ^ a)) * tall
        return pl.ds(pl.multiple_of(at, tall), tall)

    @pl.when(step == 0)
    def _():
        for a in range(planes):
            for z in range(lines):
                for h in range(heads):
                    b2[h, placed(a, z), :] = bias_refs[a][z, h].astype(jnp.float32) * LOG2E
        if first:
            db_ref[...] = jnp.zeros_like(db_ref)
        else:
            db_ref[...] = before_ref[...]

    q, k, v, g = q_ref[0], k_ref[0], v_ref[0], g_ref[0]
    qt[...] = q.T
    gt[...] = g.T
    kt = k.T
    vt = v.T
    product = g.astype(jnp.float32) * o_ref[0].astype(jnp.float32)
    lane = lax.broadcasted_iota(jnp.int32, (1, width), 1)
    ln_lane = lax.broadcasted_iota(jnp.int32, (1, ln_ref.shape[2]), 1)
    block = 256
    grad_q = [None] * (length // block)
    for h in range(heads):
        head = core * heads + h
        mine = (lane // size) == head
        ln = jnp.sum(jnp.where(ln_lane == head, ln_ref[0], 0.0), axis=1, keepdims=True) * LOG2E
        delta = jnp.sum(jnp.where(mine, product, 0.0), axis=1, keepdims=True)
        zero = jnp.zeros_like(q)
        qh = jnp.where(mine, q, zero)
        gh = jnp.where(mine, g, zero)
        kh = jnp.where(mine, k, zero)
        rows = pl.ds(pl.multiple_of(head * size, size), size)
        qth = qt[rows, :]
        gth = gt[rows, :]
        grad_k = None
        for b in range(length // block):
            span = slice(b * block, (b + 1) * block)
            s = jnp.dot(qh[span], kt, preferred_element_type=jnp.float32)
            d = jnp.dot(gh[span], vt, preferred_element_type=jnp.float32)
            p = jnp.exp2(s * (scale * LOG2E) + b2[h, span, :] - ln[span])
            ds = p * (d - delta[span])
            db_ref[h, span, :] += ds
            pb = p.astype(jnp.bfloat16)
            dsb = ds.astype(jnp.bfloat16)
            gv = jnp.dot(gth[:, span], pb, preferred_element_type=jnp.float32)
            gk = jnp.dot(qth[:, span], dsb, preferred_element_type=jnp.float32)
            gq = jnp.dot(dsb, kh, preferred_element_type=jnp.float32)
            grad_k = gk if grad_k is None else grad_k + gk
            grad_v = gv if b == 0 else grad_v + gv
            grad_q[b] = gq if grad_q[b] is None else grad_q[b] + gq
        kvt[h * size : (h + 1) * size, :] = (grad_k * scale).astype(jnp.bfloat16)
        kvt[(heads + h) * size : (heads + h + 1) * size, :] = grad_v.astype(jnp.bfloat16)
    half = heads * size
    own = pl.multiple_of(core * half, half)
    w_kv = jnp.concatenate(
        [w_ref[pl.ds(width + own, half), :], w_ref[pl.ds(2 * width + own, half), :]], axis=0
    )
    kv = kvt[...].T
    for b in range(length // block):
        span = slice(b * block, (b + 1) * block)
        total = jnp.dot(
            (grad_q[b] * scale).astype(jnp.bfloat16), w_ref[:width, :], preferred_element_type=jnp.float32
        ) + jnp.dot(kv[span], w_kv, preferred_element_type=jnp.float32)
        pair_ref[0, span, :] = total.astype(pair_ref.dtype)

    if not first:

        @pl.when(step == pl.num_programs(0) - 1)
        def _():
            for a in range(planes):
                for z in range(lines):
                    for h in range(heads):
                        wire_refs[a][z, h] = db_ref[h, placed(a, z), :].astype(wire_refs[a].dtype)


def run_rows(place, acts, bias, weight, before=None):
    first = before is None
    rows, length, width = acts[0].shape
    heads = bias[0].shape[1]
    row = pl.BlockSpec((1, length, width), lambda i: (i, 0, 0))
    whole = lambda x: pl.BlockSpec(x.shape, lambda i: (0,) * len(x.shape))
    ln = acts[-1]
    in_specs = [pl.BlockSpec(memory_space=pltpu.SMEM)] + [row] * 5
    in_specs += [pl.BlockSpec((1,) + ln.shape[1:], lambda i: (i, 0, 0)), whole(weight)]
    in_specs += [whole(x) for x in bias]
    args = [place, *acts, weight, *bias]
    square = jax.ShapeDtypeStruct((heads, length, length), jnp.float32)
    scratch = [
        pltpu.VMEM(square.shape, jnp.float32),
        pltpu.VMEM((width, length), jnp.bfloat16),
        pltpu.VMEM((width, length), jnp.bfloat16),
        pltpu.VMEM((width, length), jnp.bfloat16),
    ]
    if first:
        outs = [jax.ShapeDtypeStruct((rows, length, width), jnp.bfloat16), square]
        out_specs = [row, whole(square)]
    else:
        args.append(before)
        in_specs.append(whole(before))
        outs = [jax.ShapeDtypeStruct((rows, length, width), jnp.float32)]
        outs += [jax.ShapeDtypeStruct(x.shape, jnp.bfloat16) for x in bias]
        out_specs = [row] + [whole(x) for x in bias]
        scratch.append(pltpu.VMEM(square.shape, jnp.float32))
    return pl.pallas_call(
        functools.partial(attention_rows, first, len(bias)),
        grid=(rows,),
        in_specs=in_specs,
        out_specs=out_specs,
        out_shape=outs,
        scratch_shapes=scratch,
        compiler_params=pltpu.CompilerParams(dimension_semantics=("arbitrary",)),
        cost_estimate=pl.CostEstimate(
            flops=10 * rows * heads * length * length * width,
            bytes_accessed=8 * 1024 * 1024,
            transcendentals=rows * heads * length * length,
        ),
        name="partner_rows" if first else "own_rows",
    )(*args)


def sum_pieces(*refs):
    count = len(refs) // 2
    for z, out_ref in enumerate(refs[count:]):
        total = refs[0][z].astype(jnp.float32)
        for ref in refs[1:count]:
            total += ref[z].astype(jnp.float32)
        out_ref[...] = total.astype(out_ref.dtype)


def plane_sum(pieces):
    out = jax.ShapeDtypeStruct(pieces[0].shape[1:], pieces[0].dtype)
    return pl.pallas_call(sum_pieces, out_shape=[out] * len(pieces), name="plane_sum")(*pieces)


def local(query_act, key_act, value_act, attn_out, grad_out, pair_bias, log_norm, back_weight):
    heads, tall, length = pair_bias.shape
    lines, cores = lax.axis_size(Z), lax.axis_size(C)
    planes = lax.axis_size((Y, X))
    near = heads // cores
    core = lax.axis_index(C)
    place = jnp.stack([core, lax.axis_index(Z), lax.axis_index((Y, X))]).astype(jnp.int32)

    def heads_of(x, which):
        return lax.dynamic_slice_in_dim(x, which * near, near, 0)

    def in_core_order(mine, theirs, axis):
        lower = jnp.where(core == 0, mine, theirs)
        upper = jnp.where(core == 0, theirs, mine)
        return jnp.concatenate([lower, upper], axis)

    chip = in_core_order(heads_of(pair_bias, core), across(heads_of(pair_bias, 1 - core)), 1)
    line = jnp.stack([chip] + [swapped_with(chip, Z, m) for m in range(1, lines)])
    bias = [line] + [swapped_with(line, (Y, X), m) for m in range(1, planes)]

    own = (query_act, key_act, value_act, attn_out, grad_out, jnp.swapaxes(log_norm, 1, 2))
    other = tuple(across(x) for x in own[:5]) + (jnp.swapaxes(across(log_norm), 1, 2),)

    sent, half_sum = run_rows(place, other, bias, back_weight)
    kept, *terms = run_rows(place, own, bias, back_weight, half_sum)
    pair_rows = (kept + across(sent).astype(jnp.float32)).astype(jnp.bfloat16)
    swapped = jnp.transpose(pair_rows, (1, 0, 2))
    column_grad = lax.all_to_all(swapped, ROWS, split_axis=0, concat_axis=1, tiled=True)

    pieces = plane_sum(terms[:1] + [swapped_with(terms[m], (Y, X), m) for m in range(1, planes)])
    total = pieces[0].astype(jnp.float32)
    for m in range(1, lines):
        total += swapped_with(pieces[m], Z, m).astype(jnp.float32)

    def rows_of(x, which):
        return lax.dynamic_slice_in_dim(x, which * tall, tall, 1)

    partner = across(rows_of(total, 1 - core).astype(jnp.bfloat16)).astype(jnp.float32)
    bias_grad = in_core_order(rows_of(total, core), partner, 0)
    return (column_grad, bias_grad)


def solution(mesh):
    finer = Mesh(mesh.devices.reshape(8, 2, 4, 2, mesh.shape["dp"]), (*ROWS, "dp"))
    row = P(DP_ROWS, None, None)
    return jax.shard_map(
        local,
        mesh=finer,
        in_specs=(row, row, row, row, row, P(None, DP_ROWS, None), row, P()),
        out_specs=(P(ROWS, "dp", None), P(None, DP_ROWS, None)),
        check_vma=False,
    )
```

```python
import functools

import jax
import jax.numpy as jnp
from jax import lax
from jax.experimental import pallas as pl
from jax.experimental.pallas import tpu as pltpu
from jax.sharding import Mesh
from jax.sharding import PartitionSpec as P

Z, Y, X, C = ("rows_0", "rows_1", "rows_2", "rows_3")
ROWS = (Z, Y, X, C)
DP_ROWS = ("dp",) + ROWS
PLANE = (Y, X)
LINE = (Z, C)
SIZE = 32
LOG2E = 1.4426950408889634


def exchange(x, axes):
    return lax.all_to_all(x, axes, split_axis=0, concat_axis=0, tiled=True)


def swapped_with(x, axes, mask):
    n = lax.axis_size(axes)
    return lax.ppermute(x, axes, [(i, i ^ mask) for i in range(n)])


def across(x):
    return swapped_with(x, C, 1)


def score_rows(first, place_ref, q_ref, k_ref, v_ref, o_ref, g_ref, ln_ref, *rest):
    if first:
        e_ref, t_ref, sum_ref = rest
    else:
        before_ref, e_ref, t_ref, wire_ref, sum_ref = rest
    step = pl.program_id(0)
    heads, length = sum_ref.shape[:2]
    width = q_ref.shape[2]
    core = place_ref[0]

    @pl.when(step == 0)
    def _():
        sum_ref[...] = jnp.zeros_like(sum_ref) if first else before_ref[...]

    q, g = q_ref[0], g_ref[0]
    kt, vt = k_ref[0].T, v_ref[0].T
    product = g.astype(jnp.float32) * o_ref[0].astype(jnp.float32)
    lane = lax.broadcasted_iota(jnp.int32, (1, width), 1)
    ln_lane = lax.broadcasted_iota(jnp.int32, (1, ln_ref.shape[2]), 1)
    block = 256
    for h in range(heads):
        head = core * heads + h
        mine = (lane // SIZE) == head
        ln = jnp.sum(jnp.where(ln_lane == head, ln_ref[0], 0.0), axis=1, keepdims=True) * LOG2E
        delta = jnp.sum(jnp.where(mine, product, 0.0), axis=1, keepdims=True)
        qh = jnp.where(mine, q, jnp.zeros_like(q))
        gh = jnp.where(mine, g, jnp.zeros_like(g))
        for b in range(length // block):
            span = slice(b * block, (b + 1) * block)
            s = jnp.dot(qh[span], kt, preferred_element_type=jnp.float32)
            d = jnp.dot(gh[span], vt, preferred_element_type=jnp.float32)
            e = jnp.exp2(s * (SIZE**-0.5 * LOG2E) - ln[span])
            t = e * (d - delta[span])
            e_ref[0, h, span, :] = e.astype(e_ref.dtype)
            t_ref[0, h, span, :] = t.astype(t_ref.dtype)
            sum_ref[h, span, :] += t

    if not first:

        @pl.when(step == pl.num_programs(0) - 1)
        def _():
            planes, _, lines, tall, _ = wire_ref.shape
            for a in range(planes):
                for h in range(heads):
                    for z in range(lines):
                        at = (z * planes + a) * tall
                        wire_ref[a, h, z] = sum_ref[h, at : at + tall, :].astype(wire_ref.dtype)


def whole(x):
    return pl.BlockSpec(x.shape, lambda i: (0,) * len(x.shape))


def per_row(x):
    return pl.BlockSpec((1,) + x.shape[1:], lambda i: (i,) + (0,) * (len(x.shape) - 1))


def estimate(products, acts, heads):
    rows, length, width = acts[0].shape
    return pl.CostEstimate(
        flops=2 * products * rows * heads * length * length * width,
        bytes_accessed=8 * 1024 * 1024,
        transcendentals=rows * heads * length * length,
    )


def run_scores(place, acts, shape, before=None):
    first = before is None
    rows, length, _ = acts[0].shape
    planes, heads, lines, tall, _ = shape
    kept = jax.ShapeDtypeStruct((rows, heads, length, length), jnp.bfloat16)
    square = jax.ShapeDtypeStruct((heads, length, length), jnp.float32)
    args = [place, *acts]
    in_specs = [pl.BlockSpec(memory_space=pltpu.SMEM)] + [per_row(x) for x in acts]
    outs = [kept, kept]
    scratch = []
    if first:
        outs.append(square)
    else:
        args.append(before)
        in_specs.append(whole(before))
        outs.append(jax.ShapeDtypeStruct(shape, jnp.bfloat16))
        scratch.append(pltpu.VMEM(square.shape, jnp.float32))
    return pl.pallas_call(
        functools.partial(score_rows, first),
        grid=(rows,),
        in_specs=in_specs,
        out_specs=[per_row(kept), per_row(kept), whole(outs[2])],
        out_shape=outs,
        scratch_shapes=scratch,
        compiler_params=pltpu.CompilerParams(dimension_semantics=("arbitrary",)),
        cost_estimate=estimate(2, acts, heads),
        name="own_scores" if first else "partner_scores",
    )(*args)


def grad_rows(place_ref, e_ref, t_ref, q_ref, k_ref, g_ref, bias_ref, w_ref, pair_ref, eb, kvt, qt, gt):
    planes, heads, lines, tall, length = bias_ref.shape
    width = q_ref.shape[2]
    scale = SIZE**-0.5
    core = place_ref[0]

    @pl.when(pl.program_id(0) == 0)
    def _():
        for h in range(heads):
            for a in range(planes):
                for z in range(lines):
                    at = (z * planes + a) * tall
                    eb[h, at : at + tall, :] = jnp.exp2(bias_ref[a, h, z].astype(jnp.float32) * LOG2E)

    k = k_ref[0]
    qt[...] = q_ref[0].T
    gt[...] = g_ref[0].T
    lane = lax.broadcasted_iota(jnp.int32, (1, width), 1)
    block = 256
    grad_q = [None] * (length // block)
    for h in range(heads):
        head = core * heads + h
        kh = jnp.where((lane // SIZE) == head, k, jnp.zeros_like(k))
        rows = pl.ds(pl.multiple_of(head * SIZE, SIZE), SIZE)
        qth = qt[rows, :]
        gth = gt[rows, :]
        grad_k = grad_v = None
        for b in range(length // block):
            span = slice(b * block, (b + 1) * block)
            factor = eb[h, span, :]
            p = (e_ref[0, h, span, :].astype(jnp.float32) * factor).astype(jnp.bfloat16)
            ds = (t_ref[0, h, span, :].astype(jnp.float32) * factor).astype(jnp.bfloat16)
            gv = jnp.dot(gth[:, span], p, preferred_element_type=jnp.float32)
            gk = jnp.dot(qth[:, span], ds, preferred_element_type=jnp.float32)
            gq = jnp.dot(ds, kh, preferred_element_type=jnp.float32)
            grad_k = gk if grad_k is None else grad_k + gk
            grad_v = gv if grad_v is None else grad_v + gv
            grad_q[b] = gq if grad_q[b] is None else grad_q[b] + gq
        kvt[h * SIZE : (h + 1) * SIZE, :] = (grad_k * scale).astype(jnp.bfloat16)
        kvt[(heads + h) * SIZE : (heads + h + 1) * SIZE, :] = grad_v.astype(jnp.bfloat16)
    half = heads * SIZE
    own = pl.multiple_of(core * half, half)
    w_kv = jnp.concatenate(
        [w_ref[pl.ds(width + own, half), :], w_ref[pl.ds(2 * width + own, half), :]], axis=0
    )
    kv = kvt[...].T
    for b in range(length // block):
        span = slice(b * block, (b + 1) * block)
        total = jnp.dot(
            (grad_q[b] * scale).astype(jnp.bfloat16), w_ref[:width, :], preferred_element_type=jnp.float32
        ) + jnp.dot(kv[span], w_kv, preferred_element_type=jnp.float32)
        pair_ref[0, span, :] = total.astype(pair_ref.dtype)


def run_grads(place, scored, acts, bias, weight, dtype, name):
    rows, length, width = acts[0].shape
    heads = bias.shape[1]
    out = jax.ShapeDtypeStruct(acts[0].shape, dtype)
    swapped = pltpu.VMEM((width, length), jnp.bfloat16)
    return pl.pallas_call(
        grad_rows,
        grid=(rows,),
        in_specs=[pl.BlockSpec(memory_space=pltpu.SMEM)]
        + [per_row(x) for x in (*scored, *acts)]
        + [whole(bias), whole(weight)],
        out_specs=per_row(out),
        out_shape=out,
        scratch_shapes=[pltpu.VMEM((heads, length, length), jnp.float32)] + [swapped] * 3,
        compiler_params=pltpu.CompilerParams(dimension_semantics=("arbitrary",)),
        cost_estimate=estimate(3, acts, heads),
        name=name,
    )(place, *scored, *acts, bias, weight)


def sum_planes(place_ref, wire_ref, *out_refs):
    for m, out_ref in enumerate(out_refs):
        z = place_ref[1] ^ m
        total = wire_ref[0, :, z].astype(jnp.float32)
        for a in range(1, wire_ref.shape[0]):
            total += wire_ref[a, :, z].astype(jnp.float32)
        out_ref[...] = total.astype(out_ref.dtype)


def plane_sum(place, wire):
    planes, heads, lines, tall, length = wire.shape
    out = jax.ShapeDtypeStruct((heads, tall, length), wire.dtype)
    return pl.pallas_call(
        sum_planes,
        in_specs=[pl.BlockSpec(memory_space=pltpu.SMEM), pl.BlockSpec(memory_space=pltpu.VMEM)],
        out_shape=[out] * lines,
        name="plane_sum",
    )(place, wire)


def local(query_act, key_act, value_act, attn_out, grad_out, pair_bias, log_norm, back_weight):
    heads, tall, length = pair_bias.shape
    lines, cores = lax.axis_size(Z), lax.axis_size(C)
    planes = lax.axis_size((Y, X))
    near = heads // cores
    core = lax.axis_index(C)
    place = jnp.stack([core, lax.axis_index(Z)]).astype(jnp.int32)
    shape = (planes, near, lines, cores * tall, length)

    own = (query_act, key_act, value_act, attn_out, grad_out)
    other = tuple(across(x) for x in own)
    other_norm = across(log_norm)

    tiles = jnp.broadcast_to(
        pair_bias.reshape(1, cores, near * tall, length), (lines, cores, near * tall, length)
    )
    line = exchange(tiles.reshape(lines * cores, near * tall, length), (Z, C))
    line = line.reshape(lines, cores, near, tall, length).transpose(2, 0, 1, 3, 4)
    line = line.reshape(1, near * lines * cores * tall, length)
    bias = exchange(jnp.broadcast_to(line, (planes, *line.shape[1:])), (Y, X)).reshape(shape)

    own_e, own_t, half_sum = run_scores(place, (*own, jnp.swapaxes(log_norm, 1, 2)), shape)
    other_e, other_t, terms = run_scores(
        place, (*other, jnp.swapaxes(other_norm, 1, 2)), shape, half_sum
    )
    used = lambda x: (x[0], x[1], x[4])
    sent = run_grads(place, (other_e, other_t), used(other), bias, back_weight, jnp.bfloat16, "partner_grads")
    kept = run_grads(place, (own_e, own_t), used(own), bias, back_weight, jnp.float32, "own_grads")

    pair_rows = (kept + across(sent).astype(jnp.float32)).astype(jnp.bfloat16)
    swapped = jnp.transpose(pair_rows, (1, 0, 2))
    column_grad = lax.all_to_all(swapped, ROWS, split_axis=0, concat_axis=1, tiled=True)

    wire = exchange(terms.reshape(planes, -1, length), (Y, X)).reshape(shape)
    pieces = plane_sum(place, wire)
    total = pieces[0].astype(jnp.float32)
    for m in range(1, lines):
        total += swapped_with(pieces[m], Z, m).astype(jnp.float32)

    def rows_of(x, which):
        return lax.dynamic_slice_in_dim(x, which * tall, tall, 1)

    mine = rows_of(total, core)
    theirs = across(rows_of(total, 1 - core).astype(jnp.bfloat16)).astype(jnp.float32)
    lower = jnp.where(core == 0, mine, theirs)
    upper = jnp.where(core == 0, theirs, mine)
    bias_grad = jnp.concatenate([lower, upper], 0) * jnp.exp(pair_bias.astype(jnp.float32))
    return (column_grad, bias_grad)


def solution(mesh):
    finer = Mesh(mesh.devices.reshape(8, 2, 4, 2, mesh.shape["dp"]), (*ROWS, "dp"))
    row = P(DP_ROWS, None, None)
    return jax.shard_map(
        local,
        mesh=finer,
        in_specs=(row, row, row, row, row, P(None, DP_ROWS, None), row, P()),
        out_specs=(P(ROWS, "dp", None), P(None, DP_ROWS, None)),
        check_vma=False,
    )
```

```python
import functools

import jax
import jax.numpy as jnp
from jax import lax
from jax.experimental import pallas as pl
from jax.experimental.pallas import tpu as pltpu
from jax.sharding import Mesh
from jax.sharding import PartitionSpec as P

Z, Z0, Y, X, C = ("rows_0", "rows_1", "rows_2", "rows_3", "rows_4")
NEAR = (Z0, Y, X, C)
ROWS = (Z,) + NEAR
DP_ROWS = ("dp",) + ROWS
PLANE = (Y, X)
LINE = (Z, C)
SIZE = 32
LOG2E = 1.4426950408889634


def exchange(x, axes):
    return lax.all_to_all(x, axes, split_axis=0, concat_axis=0, tiled=True)


def swapped_with(x, axes, mask):
    n = lax.axis_size(axes)
    return lax.ppermute(x, axes, [(i, i ^ mask) for i in range(n)])


def across(x):
    return swapped_with(x, C, 1)


def placed(m, s, tall):
    groups = lax.axis_size((Z0, Y, X))
    return pl.ds(pl.multiple_of(((lax.axis_index(Z) ^ m) * groups + s) * tall, tall), tall)


def halves(lower, upper):
    cut = lower.shape[0] // 2
    first = jnp.concatenate([lower[:cut], upper[:cut]], 0)
    return first, jnp.concatenate([lower[cut:], upper[cut:]], 0)


def score_rows(first, q_ref, k_ref, v_ref, o_ref, g_ref, ln_ref, *rest):
    if first:
        e_ref, t_ref, sum_ref = rest
    else:
        before_ref, e_ref, t_ref, wire_ref, sum_ref = rest
    step = pl.program_id(0)
    heads, length = sum_ref.shape[:2]
    width = q_ref.shape[2]
    core = lax.axis_index(C)

    @pl.when(step == 0)
    def _():
        sum_ref[...] = jnp.zeros_like(sum_ref) if first else before_ref[...]

    q, g = q_ref[0], g_ref[0]
    kt, vt = k_ref[0].T, v_ref[0].T
    product = g.astype(jnp.float32) * o_ref[0].astype(jnp.float32)
    lane = lax.broadcasted_iota(jnp.int32, (1, width), 1)
    ln_rows = ln_ref[0]
    ln_columns = jnp.concatenate([ln_rows, ln_rows], 0).T
    ln_lane = lax.broadcasted_iota(jnp.int32, (1, ln_columns.shape[1]), 1)
    block = 256
    for h in range(heads):
        head = core * heads + h
        mine = (lane // SIZE) == head
        ln = jnp.sum(jnp.where(ln_lane == head, ln_columns, 0.0), axis=1, keepdims=True) * LOG2E
        delta = jnp.sum(jnp.where(mine, product, 0.0), axis=1, keepdims=True)
        qh = jnp.where(mine, q, jnp.zeros_like(q))
        gh = jnp.where(mine, g, jnp.zeros_like(g))
        for b in range(length // block):
            span = slice(b * block, (b + 1) * block)
            s = jnp.dot(qh[span], kt, preferred_element_type=jnp.float32)
            d = jnp.dot(gh[span], vt, preferred_element_type=jnp.float32)
            e = jnp.exp2(s * (SIZE**-0.5 * LOG2E) - ln[span])
            t = e * (d - delta[span])
            e_ref[0, h, span, :] = e.astype(e_ref.dtype)
            t_ref[0, h, span, :] = t.astype(t_ref.dtype)
            sum_ref[h, span, :] += t

    if not first:

        @pl.when(step == pl.num_programs(0) - 1)
        def _():
            groups, _, lines, tall, _ = wire_ref.shape
            for s in range(groups):
                for m in range(lines):
                    rows = placed(m, s, tall)
                    sides = halves(sum_ref[0, rows, :], sum_ref[1, rows, :])
                    for c, side in enumerate(sides):
                        wire_ref[s, c, m] = side.astype(wire_ref.dtype)


def whole(x):
    return pl.BlockSpec(x.shape, lambda i: (0,) * len(x.shape))


def per_row(x):
    return pl.BlockSpec((1,) + x.shape[1:], lambda i: (i,) + (0,) * (len(x.shape) - 1))


def estimate(products, acts, heads):
    rows, length, width = acts[0].shape
    return pl.CostEstimate(
        flops=2 * products * rows * heads * length * length * width,
        bytes_accessed=8 * 1024 * 1024,
        transcendentals=rows * heads * length * length,
    )


def run_scores(acts, shape, before=None):
    first = before is None
    rows, length, _ = acts[0].shape
    heads = shape[1]
    kept = jax.ShapeDtypeStruct((rows, heads, length, length), jnp.bfloat16)
    square = jax.ShapeDtypeStruct((heads, length, length), jnp.float32)
    args = [*acts]
    in_specs = [per_row(x) for x in acts]
    outs = [kept, kept]
    scratch = []
    if first:
        outs.append(square)
    else:
        args.append(before)
        in_specs.append(whole(before))
        outs.append(jax.ShapeDtypeStruct(shape, jnp.bfloat16))
        scratch.append(pltpu.VMEM(square.shape, jnp.float32))
    return pl.pallas_call(
        functools.partial(score_rows, first),
        grid=(rows,),
        in_specs=in_specs,
        out_specs=[per_row(kept), per_row(kept), whole(outs[2])],
        out_shape=outs,
        scratch_shapes=scratch,
        compiler_params=pltpu.CompilerParams(dimension_semantics=("arbitrary",)),
        cost_estimate=estimate(2, acts, heads),
        name="own_scores" if first else "partner_scores",
    )(*args)


def grad_rows(e_ref, t_ref, q_ref, k_ref, g_ref, bias_ref, w_ref, pair_ref, eb, kvt, qt, gt):
    groups, heads, lines, tall, length = bias_ref.shape
    width = q_ref.shape[2]
    scale = SIZE**-0.5
    core = lax.axis_index(C)

    @pl.when(pl.program_id(0) == 0)
    def _():
        for s in range(groups):
            for m in range(lines):
                sides = [bias_ref[s, c, m].astype(jnp.float32) for c in range(2)]
                for h, both in enumerate(halves(*sides)):
                    eb[h, placed(m, s, tall), :] = jnp.exp2(both * LOG2E)

    k = k_ref[0]
    qt[...] = q_ref[0].T
    gt[...] = g_ref[0].T
    lane = lax.broadcasted_iota(jnp.int32, (1, width), 1)
    block = 256
    grad_q = [None] * (length // block)
    for h in range(heads):
        head = core * heads + h
        kh = jnp.where((lane // SIZE) == head, k, jnp.zeros_like(k))
        rows = pl.ds(pl.multiple_of(head * SIZE, SIZE), SIZE)
        qth = qt[rows, :]
        gth = gt[rows, :]
        grad_k = grad_v = None
        for b in range(length // block):
            span = slice(b * block, (b + 1) * block)
            factor = eb[h, span, :]
            p = (e_ref[0, h, span, :].astype(jnp.float32) * factor).astype(jnp.bfloat16)
            ds = (t_ref[0, h, span, :].astype(jnp.float32) * factor).astype(jnp.bfloat16)
            gv = jnp.dot(gth[:, span], p, preferred_element_type=jnp.float32)
            gk = jnp.dot(qth[:, span], ds, preferred_element_type=jnp.float32)
            gq = jnp.dot(ds, kh, preferred_element_type=jnp.float32)
            grad_k = gk if grad_k is None else grad_k + gk
            grad_v = gv if grad_v is None else grad_v + gv
            grad_q[b] = gq if grad_q[b] is None else grad_q[b] + gq
        kvt[h * SIZE : (h + 1) * SIZE, :] = (grad_k * scale).astype(jnp.bfloat16)
        kvt[(heads + h) * SIZE : (heads + h + 1) * SIZE, :] = grad_v.astype(jnp.bfloat16)
    half = heads * SIZE
    own = pl.multiple_of(core * half, half)
    w_kv = jnp.concatenate(
        [w_ref[pl.ds(width + own, half), :], w_ref[pl.ds(2 * width + own, half), :]], axis=0
    )
    kv = kvt[...].T
    for b in range(length // block):
        span = slice(b * block, (b + 1) * block)
        total = jnp.dot(
            (grad_q[b] * scale).astype(jnp.bfloat16), w_ref[:width, :], preferred_element_type=jnp.float32
        ) + jnp.dot(kv[span], w_kv, preferred_element_type=jnp.float32)
        pair_ref[0, span, :] = total.astype(pair_ref.dtype)


def run_grads(scored, acts, bias, weight, dtype, name):
    rows, length, width = acts[0].shape
    heads = bias.shape[1]
    out = jax.ShapeDtypeStruct(acts[0].shape, dtype)
    swapped = pltpu.VMEM((width, length), jnp.bfloat16)
    return pl.pallas_call(
        grad_rows,
        grid=(rows,),
        in_specs=[per_row(x) for x in (*scored, *acts)]
        + [whole(bias), whole(weight)],
        out_specs=per_row(out),
        out_shape=out,
        scratch_shapes=[pltpu.VMEM((heads, length, length), jnp.float32)] + [swapped] * 3,
        compiler_params=pltpu.CompilerParams(dimension_semantics=("arbitrary",)),
        cost_estimate=estimate(3, acts, heads),
        name=name,
    )(*scored, *acts, bias, weight)


def sum_groups(wire_ref, *out_refs):
    tall = wire_ref.shape[3]
    for m, out_ref in enumerate(out_refs):
        for c in range(wire_ref.shape[1]):
            total = wire_ref[0, c, m].astype(jnp.float32)
            for s in range(1, wire_ref.shape[0]):
                total += wire_ref[s, c, m].astype(jnp.float32)
            out_ref[c * tall : (c + 1) * tall, :] = total.astype(out_ref.dtype)


def group_sum(wire):
    _, cores, lines, tall, length = wire.shape
    out = lambda kind: jax.ShapeDtypeStruct((cores * tall, length), kind)
    return pl.pallas_call(
        sum_groups,
        out_shape=[out(jnp.float32)] + [out(wire.dtype)] * (lines - 1),
        name="group_sum",
    )(wire)


def local(query_act, key_act, value_act, attn_out, grad_out, pair_bias, log_norm, back_weight):
    heads, tall, length = pair_bias.shape
    lines, cores = lax.axis_size(Z), lax.axis_size(C)
    groups = lax.axis_size((Z0, Y, X))
    near = heads // cores
    shape = (groups, cores, lines, near * tall, length)

    own = (query_act, key_act, value_act, attn_out, grad_out, log_norm)
    other = tuple(across(x) for x in own)

    line = jnp.stack([pair_bias] + [swapped_with(pair_bias, Z, m) for m in range(1, lines)], 1)
    line = line.reshape(1, cores, near, lines, tall, length).transpose(0, 1, 3, 2, 4, 5)
    line = line.reshape(1, cores, lines * near * tall, length)
    tiles = jnp.broadcast_to(line, (groups, *line.shape[1:])).reshape(groups * cores, -1, length)
    bias = exchange(tiles, NEAR).reshape(shape)

    own_e, own_t, half_sum = run_scores(own, shape)
    other_e, other_t, terms = run_scores(other, shape, half_sum)
    used = lambda x: (x[0], x[1], x[4])
    sent = run_grads((other_e, other_t), used(other), bias, back_weight, jnp.bfloat16, "partner_grads")
    kept = run_grads((own_e, own_t), used(own), bias, back_weight, jnp.float32, "own_grads")

    pair_rows = (kept + across(sent).astype(jnp.float32)).astype(jnp.bfloat16)
    swapped = jnp.transpose(pair_rows, (1, 0, 2))
    column_grad = lax.all_to_all(swapped, ROWS, split_axis=0, concat_axis=1, tiled=True)

    wire = exchange(terms.reshape(groups * cores, -1, length), NEAR).reshape(shape)
    total, *pieces = group_sum(wire)
    for m, piece in enumerate(pieces, 1):
        total += swapped_with(piece, Z, m).astype(jnp.float32)
    bias_grad = total.reshape(pair_bias.shape) * jnp.exp(pair_bias.astype(jnp.float32))
    return (column_grad, bias_grad)


def solution(mesh):
    finer = Mesh(mesh.devices.reshape(4, 2, 2, 4, 2, mesh.shape["dp"]), (*ROWS, "dp"))
    row = P(DP_ROWS, None, None)
    return jax.shard_map(
        local,
        mesh=finer,
        in_specs=(row, row, row, row, row, P(None, DP_ROWS, None), row, P()),
        out_specs=(P(ROWS, "dp", None), P(None, DP_ROWS, None)),
        check_vma=False,
    )
```

```python
import functools

import jax
import jax.numpy as jnp
from jax import lax
from jax.experimental import pallas as pl
from jax.experimental.pallas import tpu as pltpu
from jax.sharding import Mesh
from jax.sharding import PartitionSpec as P

Z, Z0, Y, X, C = ("rows_0", "rows_1", "rows_2", "rows_3", "rows_4")
NEAR = (Z0, Y, X, C)
ROWS = (Z,) + NEAR
DP_ROWS = ("dp",) + ROWS
PLANE = (Y, X)
LINE = (Z, C)
SIZE = 32
VMEM = 20 * 1024 * 1024
LOG2E = 1.4426950408889634


def exchange(x, axes):
    return lax.all_to_all(x, axes, split_axis=0, concat_axis=0, tiled=True)


def swapped_with(x, axes, mask):
    n = lax.axis_size(axes)
    return lax.ppermute(x, axes, [(i, i ^ mask) for i in range(n)])


def across(x):
    return swapped_with(x, C, 1)


def placed(m, s, tall):
    groups = lax.axis_size((Z0, Y, X))
    return pl.ds(pl.multiple_of(((lax.axis_index(Z) ^ m) * groups + s) * tall, tall), tall)


def halves(lower, upper):
    cut = lower.shape[0] // 2
    first = jnp.concatenate([lower[:cut], upper[:cut]], 0)
    return first, jnp.concatenate([lower[cut:], upper[cut:]], 0)


def score_rows(first, q_ref, k_ref, v_ref, o_ref, g_ref, ln_ref, *rest):
    if first:
        e_ref, t_ref, sum_ref = rest
    else:
        before_ref, e_ref, t_ref, wire_ref, sum_ref = rest
    step = pl.program_id(0)
    heads, length = sum_ref.shape[:2]
    width = q_ref.shape[2]
    core = lax.axis_index(C)

    @pl.when(step == 0)
    def _():
        sum_ref[...] = jnp.zeros_like(sum_ref) if first else before_ref[...]

    q, g = q_ref[0], g_ref[0]
    kt, vt = k_ref[0].T, v_ref[0].T
    product = g.astype(jnp.float32) * o_ref[0].astype(jnp.float32)
    lane = lax.broadcasted_iota(jnp.int32, (1, width), 1)
    ln_rows = ln_ref[0]
    ln_columns = jnp.concatenate([ln_rows, ln_rows], 0).T
    ln_lane = lax.broadcasted_iota(jnp.int32, (1, ln_columns.shape[1]), 1)
    block = 256
    for h in range(heads):
        head = core * heads + h
        mine = (lane // SIZE) == head
        ln = jnp.sum(jnp.where(ln_lane == head, ln_columns, 0.0), axis=1, keepdims=True) * LOG2E
        delta = jnp.sum(jnp.where(mine, product, 0.0), axis=1, keepdims=True)
        qh = jnp.where(mine, q, jnp.zeros_like(q))
        gh = jnp.where(mine, g, jnp.zeros_like(g))
        for b in range(length // block):
            span = slice(b * block, (b + 1) * block)
            s = jnp.dot(qh[span], kt, preferred_element_type=jnp.float32)
            d = jnp.dot(gh[span], vt, preferred_element_type=jnp.float32)
            e = jnp.exp2(s * (SIZE**-0.5 * LOG2E) - ln[span])
            t = e * (d - delta[span])
            e_ref[0, h, span, :] = e.astype(e_ref.dtype)
            t_ref[0, h, span, :] = t.astype(t_ref.dtype)
            sum_ref[h, span, :] += t

    if not first:

        @pl.when(step == pl.num_programs(0) - 1)
        def _():
            groups, _, lines, tall, _ = wire_ref.shape
            for s in range(groups):
                for m in range(lines):
                    rows = placed(m, s, tall)
                    sides = halves(sum_ref[0, rows, :], sum_ref[1, rows, :])
                    for c, side in enumerate(sides):
                        wire_ref[s, c, m] = side.astype(wire_ref.dtype)


def whole(x):
    return pl.BlockSpec(x.shape, lambda i: (0,) * len(x.shape))


def per_row(x):
    return pl.BlockSpec((1,) + x.shape[1:], lambda i: (i,) + (0,) * (len(x.shape) - 1))


def estimate(products, acts, heads):
    rows, length, width = acts[0].shape
    return pl.CostEstimate(
        flops=2 * products * rows * heads * length * length * width,
        bytes_accessed=8 * 1024 * 1024,
        transcendentals=rows * heads * length * length,
    )


def run_scores(acts, shape, before=None):
    first = before is None
    rows, length, _ = acts[0].shape
    heads = shape[1]
    kept = jax.ShapeDtypeStruct((rows, heads, length, length), jnp.bfloat16)
    square = jax.ShapeDtypeStruct((heads, length, length), jnp.float32)
    args = [*acts]
    in_specs = [per_row(x) for x in acts]
    outs = [kept, kept]
    scratch = []
    if first:
        outs.append(square)
    else:
        args.append(before)
        in_specs.append(whole(before))
        outs.append(jax.ShapeDtypeStruct(shape, jnp.bfloat16))
        scratch.append(pltpu.VMEM(square.shape, jnp.float32))
    return pl.pallas_call(
        functools.partial(score_rows, first),
        grid=(rows,),
        in_specs=in_specs,
        out_specs=[per_row(kept), per_row(kept), whole(outs[2])],
        out_shape=outs,
        scratch_shapes=scratch,
        compiler_params=pltpu.CompilerParams(dimension_semantics=("arbitrary",), vmem_limit_bytes=VMEM),
        cost_estimate=estimate(2, acts, heads),
        name="own_scores" if first else "partner_scores",
    )(*args)


def grad_rows(e_ref, t_ref, q_ref, k_ref, g_ref, bias_ref, w_ref, pair_ref, eb, kvt, qt, gt):
    groups, heads, lines, tall, length = bias_ref.shape
    width = q_ref.shape[2]
    scale = SIZE**-0.5
    core = lax.axis_index(C)

    @pl.when(pl.program_id(0) == 0)
    def _():
        for s in range(groups):
            for m in range(lines):
                sides = [bias_ref[s, c, m].astype(jnp.float32) for c in range(2)]
                for h, both in enumerate(halves(*sides)):
                    eb[h, placed(m, s, tall), :] = jnp.exp2(both * LOG2E)

    k = k_ref[0]
    qt[...] = q_ref[0].T
    gt[...] = g_ref[0].T
    lane = lax.broadcasted_iota(jnp.int32, (1, width), 1)
    block = 256
    grad_q = [None] * (length // block)
    for h in range(heads):
        head = core * heads + h
        kh = jnp.where((lane // SIZE) == head, k, jnp.zeros_like(k))
        rows = pl.ds(pl.multiple_of(head * SIZE, SIZE), SIZE)
        qth = qt[rows, :]
        gth = gt[rows, :]
        grad_k = grad_v = None
        for b in range(length // block):
            span = slice(b * block, (b + 1) * block)
            factor = eb[h, span, :]
            p = (e_ref[0, h, span, :].astype(jnp.float32) * factor).astype(jnp.bfloat16)
            ds = (t_ref[0, h, span, :].astype(jnp.float32) * factor).astype(jnp.bfloat16)
            gv = jnp.dot(gth[:, span], p, preferred_element_type=jnp.float32)
            gk = jnp.dot(qth[:, span], ds, preferred_element_type=jnp.float32)
            gq = jnp.dot(ds, kh, preferred_element_type=jnp.float32)
            grad_k = gk if grad_k is None else grad_k + gk
            grad_v = gv if grad_v is None else grad_v + gv
            grad_q[b] = gq if grad_q[b] is None else grad_q[b] + gq
        kvt[h * SIZE : (h + 1) * SIZE, :] = (grad_k * scale).astype(jnp.bfloat16)
        kvt[(heads + h) * SIZE : (heads + h + 1) * SIZE, :] = grad_v.astype(jnp.bfloat16)
    half = heads * SIZE
    own = pl.multiple_of(core * half, half)
    w_kv = jnp.concatenate(
        [w_ref[pl.ds(width + own, half), :], w_ref[pl.ds(2 * width + own, half), :]], axis=0
    )
    kv = kvt[...].T
    for b in range(length // block):
        span = slice(b * block, (b + 1) * block)
        total = jnp.dot(
            (grad_q[b] * scale).astype(jnp.bfloat16), w_ref[:width, :], preferred_element_type=jnp.float32
        ) + jnp.dot(kv[span], w_kv, preferred_element_type=jnp.float32)
        pair_ref[0, span, :] = total.astype(pair_ref.dtype)


def run_grads(scored, acts, bias, weight, dtype, name):
    rows, length, width = acts[0].shape
    heads = bias.shape[1]
    out = jax.ShapeDtypeStruct(acts[0].shape, dtype)
    swapped = pltpu.VMEM((width, length), jnp.bfloat16)
    return pl.pallas_call(
        grad_rows,
        grid=(rows,),
        in_specs=[per_row(x) for x in (*scored, *acts)]
        + [whole(bias), whole(weight)],
        out_specs=per_row(out),
        out_shape=out,
        scratch_shapes=[pltpu.VMEM((heads, length, length), jnp.float32)] + [swapped] * 3,
        compiler_params=pltpu.CompilerParams(dimension_semantics=("arbitrary",), vmem_limit_bytes=VMEM),
        cost_estimate=estimate(3, acts, heads),
        name=name,
    )(*scored, *acts, bias, weight)


def sum_groups(wire_ref, *out_refs):
    tall = wire_ref.shape[3]
    for m, out_ref in enumerate(out_refs):
        for c in range(wire_ref.shape[1]):
            total = wire_ref[0, c, m].astype(jnp.float32)
            for s in range(1, wire_ref.shape[0]):
                total += wire_ref[s, c, m].astype(jnp.float32)
            out_ref[c * tall : (c + 1) * tall, :] = total.astype(out_ref.dtype)


def group_sum(wire):
    _, cores, lines, tall, length = wire.shape
    out = lambda kind: jax.ShapeDtypeStruct((cores * tall, length), kind)
    return pl.pallas_call(
        sum_groups,
        out_shape=[out(jnp.float32)] + [out(wire.dtype)] * (lines - 1),
        name="group_sum",
    )(wire)


def local(query_act, key_act, value_act, attn_out, grad_out, pair_bias, log_norm, back_weight):
    heads, tall, length = pair_bias.shape
    lines, cores = lax.axis_size(Z), lax.axis_size(C)
    groups = lax.axis_size((Z0, Y, X))
    near = heads // cores
    shape = (groups, cores, lines, near * tall, length)

    own = (query_act, key_act, value_act, attn_out, grad_out, log_norm)
    other = tuple(across(x) for x in own)

    line = jnp.stack([pair_bias] + [swapped_with(pair_bias, Z, m) for m in range(1, lines)], 1)
    line = line.reshape(1, cores, near, lines, tall, length).transpose(0, 1, 3, 2, 4, 5)
    line = line.reshape(1, cores, lines * near * tall, length)
    tiles = jnp.broadcast_to(line, (groups, *line.shape[1:])).reshape(groups * cores, -1, length)
    bias = exchange(tiles, NEAR).reshape(shape)

    own_e, own_t, half_sum = run_scores(own, shape)
    other_e, other_t, terms = run_scores(other, shape, half_sum)
    used = lambda x: (x[0], x[1], x[4])
    sent = run_grads((other_e, other_t), used(other), bias, back_weight, jnp.bfloat16, "partner_grads")
    kept = run_grads((own_e, own_t), used(own), bias, back_weight, jnp.float32, "own_grads")

    pair_rows = (kept + across(sent).astype(jnp.float32)).astype(jnp.bfloat16)
    swapped = jnp.transpose(pair_rows, (1, 0, 2))
    column_grad = lax.all_to_all(swapped, ROWS, split_axis=0, concat_axis=1, tiled=True)

    wire = exchange(terms.reshape(groups * cores, -1, length), NEAR).reshape(shape)
    total, *pieces = group_sum(wire)
    for m, piece in enumerate(pieces, 1):
        total += swapped_with(piece, Z, m).astype(jnp.float32)
    bias_grad = total.reshape(pair_bias.shape) * jnp.exp(pair_bias.astype(jnp.float32))
    return (column_grad, bias_grad)


def solution(mesh):
    finer = Mesh(mesh.devices.reshape(4, 2, 2, 4, 2, mesh.shape["dp"]), (*ROWS, "dp"))
    row = P(DP_ROWS, None, None)
    return jax.shard_map(
        local,
        mesh=finer,
        in_specs=(row, row, row, row, row, P(None, DP_ROWS, None), row, P()),
        out_specs=(P(ROWS, "dp", None), P(None, DP_ROWS, None)),
        check_vma=False,
    )
```

```python
import functools

import jax
import jax.numpy as jnp
from jax import lax
from jax.experimental import pallas as pl
from jax.experimental.pallas import tpu as pltpu
from jax.sharding import Mesh
from jax.sharding import PartitionSpec as P

Z, Z0, Y, X, C = ("rows_0", "rows_1", "rows_2", "rows_3", "rows_4")
NEAR = (Z0, Y, X, C)
ROWS = (Z,) + NEAR
DP_ROWS = ("dp",) + ROWS
PLANE = (Y, X)
LINE = (Z, C)
SIZE = 32
VMEM = 20 * 1024 * 1024
LOG2E = 1.4426950408889634


def exchange(x, axes):
    return lax.all_to_all(x, axes, split_axis=0, concat_axis=0, tiled=True)


def swapped_with(x, axes, mask):
    n = lax.axis_size(axes)
    return lax.ppermute(x, axes, [(i, i ^ mask) for i in range(n)])


def across(x):
    return swapped_with(x, C, 1)


def placed(m, s, tall):
    groups = lax.axis_size((Z0, Y, X))
    return pl.ds(pl.multiple_of(((lax.axis_index(Z) ^ m) * groups + s) * tall, tall), tall)


def halves(lower, upper):
    cut = lower.shape[0] // 2
    first = jnp.concatenate([lower[:cut], upper[:cut]], 0)
    return first, jnp.concatenate([lower[cut:], upper[cut:]], 0)


def score_rows(first, q_ref, k_ref, v_ref, o_ref, g_ref, ln_ref, *rest):
    if first:
        (sum_ref,) = rest
    else:
        before_ref, wire_ref, sum_ref = rest
    step = pl.program_id(0)
    heads, length = sum_ref.shape[:2]
    width = q_ref.shape[2]
    core = lax.axis_index(C)

    @pl.when(step == 0)
    def _():
        sum_ref[...] = jnp.zeros_like(sum_ref) if first else before_ref[...]

    q, g = q_ref[0], g_ref[0]
    kt, vt = k_ref[0].T, v_ref[0].T
    product = g.astype(jnp.float32) * o_ref[0].astype(jnp.float32)
    lane = lax.broadcasted_iota(jnp.int32, (1, width), 1)
    ln_rows = ln_ref[0]
    ln_columns = jnp.concatenate([ln_rows, ln_rows], 0).T
    ln_lane = lax.broadcasted_iota(jnp.int32, (1, ln_columns.shape[1]), 1)
    block = 512
    for h in range(heads):
        head = core * heads + h
        mine = (lane // SIZE) == head
        ln = jnp.sum(jnp.where(ln_lane == head, ln_columns, 0.0), axis=1, keepdims=True) * LOG2E
        delta = jnp.sum(jnp.where(mine, product, 0.0), axis=1, keepdims=True)
        qh = jnp.where(mine, q, jnp.zeros_like(q))
        gh = jnp.where(mine, g, jnp.zeros_like(g))
        for b in range(length // block):
            span = slice(b * block, (b + 1) * block)
            s = jnp.dot(qh[span], kt, preferred_element_type=jnp.float32)
            d = jnp.dot(gh[span], vt, preferred_element_type=jnp.float32)
            e = jnp.exp2(s * (SIZE**-0.5 * LOG2E) - ln[span])
            sum_ref[h, span, :] += e * (d - delta[span])

    if not first:

        @pl.when(step == pl.num_programs(0) - 1)
        def _():
            groups, _, lines, tall, _ = wire_ref.shape
            for s in range(groups):
                for m in range(lines):
                    rows = placed(m, s, tall)
                    sides = halves(sum_ref[0, rows, :], sum_ref[1, rows, :])
                    for c, side in enumerate(sides):
                        wire_ref[s, c, m] = side.astype(wire_ref.dtype)


def whole(x):
    return pl.BlockSpec(x.shape, lambda i: (0,) * len(x.shape))


def per_row(x):
    return pl.BlockSpec((1,) + x.shape[1:], lambda i: (i,) + (0,) * (len(x.shape) - 1))


def estimate(products, acts, heads):
    rows, length, width = acts[0].shape
    return pl.CostEstimate(
        flops=2 * products * rows * heads * length * length * width,
        bytes_accessed=8 * 1024 * 1024,
        transcendentals=rows * heads * length * length,
    )


def run_scores(acts, shape, before=None):
    first = before is None
    rows, length, _ = acts[0].shape
    heads = shape[1]
    square = jax.ShapeDtypeStruct((heads, length, length), jnp.float32)
    args = [*acts]
    in_specs = [per_row(x) for x in acts]
    outs = []
    scratch = []
    if first:
        outs.append(square)
    else:
        args.append(before)
        in_specs.append(whole(before))
        outs.append(jax.ShapeDtypeStruct(shape, jnp.bfloat16))
        scratch.append(pltpu.VMEM(square.shape, jnp.float32))
    return pl.pallas_call(
        functools.partial(score_rows, first),
        grid=(rows,),
        in_specs=in_specs,
        out_specs=whole(outs[0]),
        out_shape=outs[0],
        scratch_shapes=scratch,
        compiler_params=pltpu.CompilerParams(dimension_semantics=("arbitrary",), vmem_limit_bytes=VMEM),
        cost_estimate=estimate(2, acts, heads),
        name="own_scores" if first else "partner_scores",
    )(*args)


def grad_rows(q_ref, k_ref, v_ref, o_ref, g_ref, ln_ref, bias_ref, w_ref, pair_ref, b2, kvt, qt, gt):
    groups, heads, lines, tall, length = bias_ref.shape
    width = q_ref.shape[2]
    scale = SIZE**-0.5
    core = lax.axis_index(C)

    @pl.when(pl.program_id(0) == 0)
    def _():
        for s in range(groups):
            for m in range(lines):
                sides = [bias_ref[s, c, m].astype(jnp.float32) for c in range(2)]
                for h, both in enumerate(halves(*sides)):
                    b2[h, placed(m, s, tall), :] = both * LOG2E

    q, k, g = q_ref[0], k_ref[0], g_ref[0]
    qt[...] = q.T
    gt[...] = g.T
    kt, vt = k.T, v_ref[0].T
    product = g.astype(jnp.float32) * o_ref[0].astype(jnp.float32)
    lane = lax.broadcasted_iota(jnp.int32, (1, width), 1)
    ln_rows = ln_ref[0]
    ln_columns = jnp.concatenate([ln_rows, ln_rows], 0).T
    ln_lane = lax.broadcasted_iota(jnp.int32, (1, ln_columns.shape[1]), 1)
    block = 512
    grad_q = [None] * (length // block)
    for h in range(heads):
        head = core * heads + h
        mine = (lane // SIZE) == head
        ln = jnp.sum(jnp.where(ln_lane == head, ln_columns, 0.0), axis=1, keepdims=True) * LOG2E
        delta = jnp.sum(jnp.where(mine, product, 0.0), axis=1, keepdims=True)
        qh = jnp.where(mine, q, jnp.zeros_like(q))
        gh = jnp.where(mine, g, jnp.zeros_like(g))
        kh = jnp.where(mine, k, jnp.zeros_like(k))
        rows = pl.ds(pl.multiple_of(head * SIZE, SIZE), SIZE)
        qth = qt[rows, :]
        gth = gt[rows, :]
        grad_k = grad_v = None
        for b in range(length // block):
            span = slice(b * block, (b + 1) * block)
            s = jnp.dot(qh[span], kt, preferred_element_type=jnp.float32)
            d = jnp.dot(gh[span], vt, preferred_element_type=jnp.float32)
            prob = jnp.exp2(s * (SIZE**-0.5 * LOG2E) + b2[h, span, :] - ln[span])
            p = prob.astype(jnp.bfloat16)
            ds = (prob * (d - delta[span])).astype(jnp.bfloat16)
            gv = jnp.dot(gth[:, span], p, preferred_element_type=jnp.float32)
            gk = jnp.dot(qth[:, span], ds, preferred_element_type=jnp.float32)
            gq = jnp.dot(ds, kh, preferred_element_type=jnp.float32)
            grad_k = gk if grad_k is None else grad_k + gk
            grad_v = gv if grad_v is None else grad_v + gv
            grad_q[b] = gq if grad_q[b] is None else grad_q[b] + gq
        kvt[h * SIZE : (h + 1) * SIZE, :] = (grad_k * scale).astype(jnp.bfloat16)
        kvt[(heads + h) * SIZE : (heads + h + 1) * SIZE, :] = grad_v.astype(jnp.bfloat16)
    half = heads * SIZE
    own = pl.multiple_of(core * half, half)
    w_kv = jnp.concatenate(
        [w_ref[pl.ds(width + own, half), :], w_ref[pl.ds(2 * width + own, half), :]], axis=0
    )
    kv = kvt[...].T
    for b in range(length // block):
        span = slice(b * block, (b + 1) * block)
        total = jnp.dot(
            (grad_q[b] * scale).astype(jnp.bfloat16), w_ref[:width, :], preferred_element_type=jnp.float32
        ) + jnp.dot(kv[span], w_kv, preferred_element_type=jnp.float32)
        pair_ref[0, span, :] = total.astype(pair_ref.dtype)


def run_grads(acts, bias, weight, dtype, name):
    rows, length, width = acts[0].shape
    heads = bias.shape[1]
    out = jax.ShapeDtypeStruct(acts[0].shape, dtype)
    swapped = pltpu.VMEM((width, length), jnp.bfloat16)
    return pl.pallas_call(
        grad_rows,
        grid=(rows,),
        in_specs=[per_row(x) for x in acts]
        + [whole(bias), whole(weight)],
        out_specs=per_row(out),
        out_shape=out,
        scratch_shapes=[pltpu.VMEM((heads, length, length), jnp.float32)] + [swapped] * 3,
        compiler_params=pltpu.CompilerParams(dimension_semantics=("arbitrary",), vmem_limit_bytes=VMEM),
        cost_estimate=estimate(5, acts, heads),
        name=name,
    )(*acts, bias, weight)


def sum_groups(wire_ref, *out_refs):
    tall = wire_ref.shape[3]
    for m, out_ref in enumerate(out_refs):
        for c in range(wire_ref.shape[1]):
            total = wire_ref[0, c, m].astype(jnp.float32)
            for s in range(1, wire_ref.shape[0]):
                total += wire_ref[s, c, m].astype(jnp.float32)
            out_ref[c * tall : (c + 1) * tall, :] = total.astype(out_ref.dtype)


def group_sum(wire):
    _, cores, lines, tall, length = wire.shape
    out = lambda kind: jax.ShapeDtypeStruct((cores * tall, length), kind)
    return pl.pallas_call(
        sum_groups,
        out_shape=[out(jnp.float32)] + [out(wire.dtype)] * (lines - 1),
        name="group_sum",
    )(wire)


def local(query_act, key_act, value_act, attn_out, grad_out, pair_bias, log_norm, back_weight):
    heads, tall, length = pair_bias.shape
    lines, cores = lax.axis_size(Z), lax.axis_size(C)
    groups = lax.axis_size((Z0, Y, X))
    near = heads // cores
    shape = (groups, cores, lines, near * tall, length)

    own = (query_act, key_act, value_act, attn_out, grad_out, log_norm)
    other = tuple(across(x) for x in own)

    line = jnp.stack([pair_bias] + [swapped_with(pair_bias, Z, m) for m in range(1, lines)], 1)
    line = line.reshape(1, cores, near, lines, tall, length).transpose(0, 1, 3, 2, 4, 5)
    line = line.reshape(1, cores, lines * near * tall, length)
    tiles = jnp.broadcast_to(line, (groups, *line.shape[1:])).reshape(groups * cores, -1, length)
    bias = exchange(tiles, NEAR).reshape(shape)

    terms = run_scores(other, shape, run_scores(own, shape))
    sent = run_grads(other, bias, back_weight, jnp.bfloat16, "partner_grads")
    kept = run_grads(own, bias, back_weight, jnp.float32, "own_grads")

    pair_rows = (kept + across(sent).astype(jnp.float32)).astype(jnp.bfloat16)
    swapped = jnp.transpose(pair_rows, (1, 0, 2))
    column_grad = lax.all_to_all(swapped, ROWS, split_axis=0, concat_axis=1, tiled=True)

    wire = exchange(terms.reshape(groups * cores, -1, length), NEAR).reshape(shape)
    total, *pieces = group_sum(wire)
    for m, piece in enumerate(pieces, 1):
        total += swapped_with(piece, Z, m).astype(jnp.float32)
    bias_grad = total.reshape(pair_bias.shape) * jnp.exp(pair_bias.astype(jnp.float32))
    return (column_grad, bias_grad)


def solution(mesh):
    finer = Mesh(mesh.devices.reshape(4, 2, 2, 4, 2, mesh.shape["dp"]), (*ROWS, "dp"))
    row = P(DP_ROWS, None, None)
    return jax.shard_map(
        local,
        mesh=finer,
        in_specs=(row, row, row, row, row, P(None, DP_ROWS, None), row, P()),
        out_specs=(P(ROWS, "dp", None), P(None, DP_ROWS, None)),
        check_vma=False,
    )
```

```python
import functools

import jax
import jax.numpy as jnp
from jax import lax
from jax.experimental import pallas as pl
from jax.experimental.pallas import tpu as pltpu
from jax.sharding import Mesh
from jax.sharding import PartitionSpec as P

Z, Z0, Y, X, C = ("rows_0", "rows_1", "rows_2", "rows_3", "rows_4")
NEAR = (Z0, Y, X, C)
ROWS = (Z,) + NEAR
DP_ROWS = ("dp",) + ROWS
PLANE = (Y, X)
LINE = (Z, C)
SIZE = 32
VMEM = 20 * 1024 * 1024
LOG2E = 1.4426950408889634


def exchange(x, axes):
    return lax.all_to_all(x, axes, split_axis=0, concat_axis=0, tiled=True)


def swapped_with(x, axes, mask):
    n = lax.axis_size(axes)
    return lax.ppermute(x, axes, [(i, i ^ mask) for i in range(n)])


def across(x):
    return swapped_with(x, C, 1)


def placed(m, s, tall):
    groups = lax.axis_size((Z0, Y, X))
    return pl.ds(pl.multiple_of(((lax.axis_index(Z) ^ m) * groups + s) * tall, tall), tall)


def halves(lower, upper):
    cut = lower.shape[0] // 2
    first = jnp.concatenate([lower[:cut], upper[:cut]], 0)
    return first, jnp.concatenate([lower[cut:], upper[cut:]], 0)


def score_rows(first, q_ref, k_ref, v_ref, o_ref, g_ref, ln_ref, *rest):
    if first:
        (sum_ref,) = rest
    else:
        before_ref, wire_ref, sum_ref = rest
    step = pl.program_id(0)
    heads, length = sum_ref.shape[:2]
    width = q_ref.shape[2]
    core = lax.axis_index(C)

    @pl.when(step == 0)
    def _():
        sum_ref[...] = jnp.zeros_like(sum_ref) if first else before_ref[...]

    q, g = q_ref[0], g_ref[0]
    kt, vt = k_ref[0].T, v_ref[0].T
    product = g.astype(jnp.float32) * o_ref[0].astype(jnp.float32)
    lane = lax.broadcasted_iota(jnp.int32, (1, width), 1)
    ln_rows = ln_ref[0]
    ln_columns = jnp.concatenate([ln_rows, ln_rows], 0).T
    ln_lane = lax.broadcasted_iota(jnp.int32, (1, ln_columns.shape[1]), 1)
    block = 512
    for h in range(heads):
        head = core * heads + h
        mine = (lane // SIZE) == head
        ln = jnp.sum(jnp.where(ln_lane == head, ln_columns, 0.0), axis=1, keepdims=True) * LOG2E
        delta = jnp.sum(jnp.where(mine, product, 0.0), axis=1, keepdims=True)
        qh = jnp.where(mine, q, jnp.zeros_like(q))
        gh = jnp.where(mine, g, jnp.zeros_like(g))
        for b in range(length // block):
            span = slice(b * block, (b + 1) * block)
            s = jnp.dot(qh[span], kt, preferred_element_type=jnp.float32)
            d = jnp.dot(gh[span], vt, preferred_element_type=jnp.float32)
            e = jnp.exp2(s * (SIZE**-0.5 * LOG2E) - ln[span])
            sum_ref[h, span, :] += e * (d - delta[span])

    if not first:

        @pl.when(step == pl.num_programs(0) - 1)
        def _():
            groups, _, lines, tall, _ = wire_ref.shape
            for s in range(groups):
                for m in range(lines):
                    rows = placed(m, s, tall)
                    sides = halves(sum_ref[0, rows, :], sum_ref[1, rows, :])
                    for c, side in enumerate(sides):
                        wire_ref[s, c, m] = side.astype(wire_ref.dtype)


def whole(x):
    return pl.BlockSpec(x.shape, lambda i: (0,) * len(x.shape))


def per_row(x):
    return pl.BlockSpec((1,) + x.shape[1:], lambda i: (i,) + (0,) * (len(x.shape) - 1))


def estimate(products, acts, heads):
    rows, length, width = acts[0].shape
    return pl.CostEstimate(
        flops=2 * products * rows * heads * length * length * width,
        bytes_accessed=8 * 1024 * 1024,
        transcendentals=rows * heads * length * length,
    )


def run_scores(acts, shape, before=None):
    first = before is None
    rows, length, _ = acts[0].shape
    heads = shape[1]
    square = jax.ShapeDtypeStruct((heads, length, length), jnp.float32)
    args = [*acts]
    in_specs = [per_row(x) for x in acts]
    outs = []
    scratch = []
    if first:
        outs.append(square)
    else:
        args.append(before)
        in_specs.append(whole(before))
        outs.append(jax.ShapeDtypeStruct(shape, jnp.bfloat16))
        scratch.append(pltpu.VMEM(square.shape, jnp.float32))
    return pl.pallas_call(
        functools.partial(score_rows, first),
        grid=(rows,),
        in_specs=in_specs,
        out_specs=whole(outs[0]),
        out_shape=outs[0],
        scratch_shapes=scratch,
        compiler_params=pltpu.CompilerParams(dimension_semantics=("arbitrary",), vmem_limit_bytes=VMEM),
        cost_estimate=estimate(2, acts, heads),
        name="own_scores" if first else "partner_scores",
    )(*args)


def grad_rows(q_ref, k_ref, v_ref, o_ref, g_ref, ln_ref, bias_ref, w_ref, pair_ref, b2, kvt, qt, gt):
    groups, heads, lines, tall, length = bias_ref.shape
    width = q_ref.shape[2]
    scale = SIZE**-0.5
    core = lax.axis_index(C)

    @pl.when(pl.program_id(0) == 0)
    def _():
        for s in range(groups):
            for m in range(lines):
                sides = [bias_ref[s, c, m].astype(jnp.float32) for c in range(2)]
                for h, both in enumerate(halves(*sides)):
                    b2[h, placed(m, s, tall), :] = both * LOG2E

    q, k, g = q_ref[0], k_ref[0], g_ref[0]
    qt[...] = q.T
    gt[...] = g.T
    kt, vt = k.T, v_ref[0].T
    product = g.astype(jnp.float32) * o_ref[0].astype(jnp.float32)
    lane = lax.broadcasted_iota(jnp.int32, (1, width), 1)
    ln_rows = ln_ref[0]
    ln_columns = jnp.concatenate([ln_rows, ln_rows], 0).T
    ln_lane = lax.broadcasted_iota(jnp.int32, (1, ln_columns.shape[1]), 1)
    block = 512
    grad_q = [None] * (length // block)
    for h in range(heads):
        head = core * heads + h
        mine = (lane // SIZE) == head
        ln = jnp.sum(jnp.where(ln_lane == head, ln_columns, 0.0), axis=1, keepdims=True) * LOG2E
        delta = jnp.sum(jnp.where(mine, product, 0.0), axis=1, keepdims=True)
        qh = jnp.where(mine, q, jnp.zeros_like(q))
        gh = jnp.where(mine, g, jnp.zeros_like(g))
        kh = jnp.where(mine, k, jnp.zeros_like(k))
        rows = pl.ds(pl.multiple_of(head * SIZE, SIZE), SIZE)
        qth = qt[rows, :]
        gth = gt[rows, :]
        grad_k = grad_v = None
        for b in range(length // block):
            span = slice(b * block, (b + 1) * block)
            s = jnp.dot(qh[span], kt, preferred_element_type=jnp.float32)
            d = jnp.dot(gh[span], vt, preferred_element_type=jnp.float32)
            prob = jnp.exp2(s * (SIZE**-0.5 * LOG2E) + b2[h, span, :] - ln[span])
            p = prob.astype(jnp.bfloat16)
            ds = (prob * (d - delta[span])).astype(jnp.bfloat16)
            gv = jnp.dot(gth[:, span], p, preferred_element_type=jnp.float32)
            gk = jnp.dot(qth[:, span], ds, preferred_element_type=jnp.float32)
            gq = jnp.dot(ds, kh, preferred_element_type=jnp.float32)
            grad_k = gk if grad_k is None else grad_k + gk
            grad_v = gv if grad_v is None else grad_v + gv
            grad_q[b] = gq if grad_q[b] is None else grad_q[b] + gq
        kvt[h * SIZE : (h + 1) * SIZE, :] = (grad_k * scale).astype(jnp.bfloat16)
        kvt[(heads + h) * SIZE : (heads + h + 1) * SIZE, :] = grad_v.astype(jnp.bfloat16)
    half = heads * SIZE
    own = pl.multiple_of(core * half, half)
    w_kv = jnp.concatenate(
        [w_ref[pl.ds(width + own, half), :], w_ref[pl.ds(2 * width + own, half), :]], axis=0
    )
    kv = kvt[...].T
    for b in range(length // block):
        span = slice(b * block, (b + 1) * block)
        total = jnp.dot(
            (grad_q[b] * scale).astype(jnp.bfloat16), w_ref[:width, :], preferred_element_type=jnp.float32
        ) + jnp.dot(kv[span], w_kv, preferred_element_type=jnp.float32)
        pair_ref[0, span, :] = total.astype(pair_ref.dtype)


def run_grads(acts, bias, weight, dtype, name):
    rows, length, width = acts[0].shape
    heads = bias.shape[1]
    out = jax.ShapeDtypeStruct(acts[0].shape, dtype)
    swapped = pltpu.VMEM((width, length), jnp.bfloat16)
    return pl.pallas_call(
        grad_rows,
        grid=(rows,),
        in_specs=[per_row(x) for x in acts]
        + [whole(bias), whole(weight)],
        out_specs=per_row(out),
        out_shape=out,
        scratch_shapes=[pltpu.VMEM((heads, length, length), jnp.float32)] + [swapped] * 3,
        compiler_params=pltpu.CompilerParams(dimension_semantics=("arbitrary",), vmem_limit_bytes=VMEM),
        cost_estimate=estimate(5, acts, heads),
        name=name,
    )(*acts, bias, weight)


def sum_groups(wire_ref, *out_refs):
    tall = wire_ref.shape[3]
    for m, out_ref in enumerate(out_refs):
        for c in range(wire_ref.shape[1]):
            total = wire_ref[0, c, m].astype(jnp.float32)
            for s in range(1, wire_ref.shape[0]):
                total += wire_ref[s, c, m].astype(jnp.float32)
            out_ref[c * tall : (c + 1) * tall, :] = total.astype(out_ref.dtype)


def group_sum(wire):
    _, cores, lines, tall, length = wire.shape
    out = lambda kind: jax.ShapeDtypeStruct((cores * tall, length), kind)
    return pl.pallas_call(
        sum_groups,
        out_shape=[out(jnp.float32)] + [out(wire.dtype)] * (lines - 1),
        name="group_sum",
    )(wire)


def local(query_act, key_act, value_act, attn_out, grad_out, pair_bias, log_norm, back_weight):
    heads, tall, length = pair_bias.shape
    lines, cores = lax.axis_size(Z), lax.axis_size(C)
    groups = lax.axis_size((Z0, Y, X))
    near = heads // cores
    shape = (groups, cores, lines, near * tall, length)

    own = (query_act, key_act, value_act, attn_out, grad_out, log_norm)
    other = tuple(across(x) for x in own)

    line = jnp.stack([pair_bias] + [swapped_with(pair_bias, Z, m) for m in range(1, lines)], 1)
    line = line.reshape(1, cores, near, lines, tall, length).transpose(0, 1, 3, 2, 4, 5)
    line = line.reshape(1, cores, lines * near * tall, length)
    tiles = jnp.broadcast_to(line, (groups, *line.shape[1:])).reshape(groups * cores, -1, length)
    bias = exchange(tiles, NEAR).reshape(shape)

    terms = run_scores(other, shape, run_scores(own, shape))
    off_chip = tuple(pltpu.with_memory_space_constraint(x, pltpu.HBM) for x in other)
    sent = run_grads(off_chip, bias, back_weight, jnp.bfloat16, "partner_grads")
    kept = run_grads(own, bias, back_weight, jnp.float32, "own_grads")

    pair_rows = (kept + across(sent).astype(jnp.float32)).astype(jnp.bfloat16)
    swapped = jnp.transpose(pair_rows, (1, 0, 2))
    column_grad = lax.all_to_all(swapped, ROWS, split_axis=0, concat_axis=1, tiled=True)

    wire = exchange(terms.reshape(groups * cores, -1, length), NEAR).reshape(shape)
    total, *pieces = group_sum(wire)
    for m, piece in enumerate(pieces, 1):
        total += swapped_with(piece, Z, m).astype(jnp.float32)
    bias_grad = total.reshape(pair_bias.shape) * jnp.exp(pair_bias.astype(jnp.float32))
    return (column_grad, bias_grad)


def solution(mesh):
    finer = Mesh(mesh.devices.reshape(4, 2, 2, 4, 2, mesh.shape["dp"]), (*ROWS, "dp"))
    row = P(DP_ROWS, None, None)
    return jax.shard_map(
        local,
        mesh=finer,
        in_specs=(row, row, row, row, row, P(None, DP_ROWS, None), row, P()),
        out_specs=(P(ROWS, "dp", None), P(None, DP_ROWS, None)),
        check_vma=False,
    )
```

```python
import functools

import jax
import jax.numpy as jnp
from jax import lax
from jax.experimental import pallas as pl
from jax.experimental.pallas import tpu as pltpu
from jax.sharding import Mesh
from jax.sharding import PartitionSpec as P

Z, Z0, Y, X, C = ("rows_0", "rows_1", "rows_2", "rows_3", "rows_4")
NEAR = (Z0, Y, X, C)
ROWS = (Z,) + NEAR
DP_ROWS = ("dp",) + ROWS
PLANE = (Y, X)
LINE = (Z, C)
SIZE = 32
VMEM = 20 * 1024 * 1024
LOG2E = 1.4426950408889634


def exchange(x, axes):
    return lax.all_to_all(x, axes, split_axis=0, concat_axis=0, tiled=True)


def swapped_with(x, axes, mask):
    n = lax.axis_size(axes)
    return lax.ppermute(x, axes, [(i, i ^ mask) for i in range(n)])


def across(x):
    return swapped_with(x, C, 1)


def placed(m, s, tall):
    groups = lax.axis_size((Z0, Y, X))
    return pl.ds(pl.multiple_of(((lax.axis_index(Z) ^ m) * groups + s) * tall, tall), tall)


def halves(lower, upper):
    cut = lower.shape[0] // 2
    first = jnp.concatenate([lower[:cut], upper[:cut]], 0)
    return first, jnp.concatenate([lower[cut:], upper[cut:]], 0)


def score_rows(first, q_ref, k_ref, v_ref, o_ref, g_ref, ln_ref, *rest):
    if first:
        (sum_ref,) = rest
    else:
        before_ref, wire_ref, sum_ref = rest
    step = pl.program_id(0)
    heads, length = sum_ref.shape[:2]
    width = q_ref.shape[2]
    core = lax.axis_index(C)

    @pl.when(step == 0)
    def _():
        sum_ref[...] = jnp.zeros_like(sum_ref) if first else before_ref[...]

    q, g = q_ref[0], g_ref[0]
    kt, vt = k_ref[0].T, v_ref[0].T
    product = g.astype(jnp.float32) * o_ref[0].astype(jnp.float32)
    lane = lax.broadcasted_iota(jnp.int32, (1, width), 1)
    ln_rows = ln_ref[0]
    ln_columns = jnp.concatenate([ln_rows, ln_rows], 0).T
    ln_lane = lax.broadcasted_iota(jnp.int32, (1, ln_columns.shape[1]), 1)
    block = 512
    for h in range(heads):
        head = core * heads + h
        mine = (lane // SIZE) == head
        ln = jnp.sum(jnp.where(ln_lane == head, ln_columns, 0.0), axis=1, keepdims=True) * LOG2E
        delta = jnp.sum(jnp.where(mine, product, 0.0), axis=1, keepdims=True)
        qh = jnp.where(mine, q, jnp.zeros_like(q))
        gh = jnp.where(mine, g, jnp.zeros_like(g))
        for b in range(length // block):
            span = slice(b * block, (b + 1) * block)
            s = jnp.dot(qh[span], kt, preferred_element_type=jnp.float32)
            d = jnp.dot(gh[span], vt, preferred_element_type=jnp.float32)
            e = jnp.exp2(s * (SIZE**-0.5 * LOG2E) - ln[span])
            sum_ref[h, span, :] += e * (d - delta[span])

    if not first:

        @pl.when(step == pl.num_programs(0) - 1)
        def _():
            groups, _, lines, tall, _ = wire_ref.shape
            for s in range(groups):
                for m in range(lines):
                    rows = placed(m, s, tall)
                    sides = halves(sum_ref[0, rows, :], sum_ref[1, rows, :])
                    for c, side in enumerate(sides):
                        wire_ref[s, c, m] = side.astype(wire_ref.dtype)


def whole(x):
    return pl.BlockSpec(x.shape, lambda i: (0,) * len(x.shape))


def per_row(x):
    return pl.BlockSpec((1,) + x.shape[1:], lambda i: (i,) + (0,) * (len(x.shape) - 1))


def estimate(products, acts, heads):
    rows, length, width = acts[0].shape
    return pl.CostEstimate(
        flops=2 * products * rows * heads * length * length * width,
        bytes_accessed=8 * 1024 * 1024,
        transcendentals=rows * heads * length * length,
    )


def run_scores(acts, shape, before=None):
    first = before is None
    rows, length, _ = acts[0].shape
    heads = shape[1]
    square = jax.ShapeDtypeStruct((heads, length, length), jnp.float32)
    args = [*acts]
    in_specs = [per_row(x) for x in acts]
    outs = []
    scratch = []
    if first:
        outs.append(square)
    else:
        args.append(before)
        in_specs.append(whole(before))
        outs.append(jax.ShapeDtypeStruct(shape, jnp.bfloat16))
        scratch.append(pltpu.VMEM(square.shape, jnp.float32))
    return pl.pallas_call(
        functools.partial(score_rows, first),
        grid=(rows,),
        in_specs=in_specs,
        out_specs=whole(outs[0]),
        out_shape=outs[0],
        scratch_shapes=scratch,
        compiler_params=pltpu.CompilerParams(dimension_semantics=("arbitrary",), vmem_limit_bytes=VMEM),
        cost_estimate=estimate(2, acts, heads),
        name="own_scores" if first else "partner_scores",
    )(*args)


def grad_rows(q_ref, k_ref, v_ref, o_ref, g_ref, ln_ref, bias_ref, w_ref, pair_ref, b2, kvt, qt, gt):
    groups, heads, lines, tall, length = bias_ref.shape
    width = q_ref.shape[2]
    scale = SIZE**-0.5
    core = lax.axis_index(C)

    @pl.when(pl.program_id(0) == 0)
    def _():
        for s in range(groups):
            for m in range(lines):
                sides = [bias_ref[s, c, m].astype(jnp.float32) for c in range(2)]
                for h, both in enumerate(halves(*sides)):
                    b2[h, placed(m, s, tall), :] = both * LOG2E

    q, k, g = q_ref[0], k_ref[0], g_ref[0]
    qt[...] = q.T
    gt[...] = g.T
    kt, vt = k.T, v_ref[0].T
    product = g.astype(jnp.float32) * o_ref[0].astype(jnp.float32)
    lane = lax.broadcasted_iota(jnp.int32, (1, width), 1)
    ln_rows = ln_ref[0]
    ln_columns = jnp.concatenate([ln_rows, ln_rows], 0).T
    ln_lane = lax.broadcasted_iota(jnp.int32, (1, ln_columns.shape[1]), 1)
    block = 512
    grad_q = [None] * (length // block)
    for h in range(heads):
        head = core * heads + h
        mine = (lane // SIZE) == head
        ln = jnp.sum(jnp.where(ln_lane == head, ln_columns, 0.0), axis=1, keepdims=True) * LOG2E
        delta = jnp.sum(jnp.where(mine, product, 0.0), axis=1, keepdims=True)
        qh = jnp.where(mine, q, jnp.zeros_like(q))
        gh = jnp.where(mine, g, jnp.zeros_like(g))
        kh = jnp.where(mine, k, jnp.zeros_like(k))
        rows = pl.ds(pl.multiple_of(head * SIZE, SIZE), SIZE)
        qth = qt[rows, :]
        gth = gt[rows, :]
        grad_k = grad_v = None
        for b in range(length // block):
            span = slice(b * block, (b + 1) * block)
            s = jnp.dot(qh[span], kt, preferred_element_type=jnp.float32)
            d = jnp.dot(gh[span], vt, preferred_element_type=jnp.float32)
            prob = jnp.exp2(s * (SIZE**-0.5 * LOG2E) + b2[h, span, :] - ln[span])
            p = prob.astype(jnp.bfloat16)
            ds = (prob * (d - delta[span])).astype(jnp.bfloat16)
            gv = jnp.dot(gth[:, span], p, preferred_element_type=jnp.float32)
            gk = jnp.dot(qth[:, span], ds, preferred_element_type=jnp.float32)
            gq = jnp.dot(ds, kh, preferred_element_type=jnp.float32)
            grad_k = gk if grad_k is None else grad_k + gk
            grad_v = gv if grad_v is None else grad_v + gv
            grad_q[b] = gq if grad_q[b] is None else grad_q[b] + gq
        kvt[h * SIZE : (h + 1) * SIZE, :] = (grad_k * scale).astype(jnp.bfloat16)
        kvt[(heads + h) * SIZE : (heads + h + 1) * SIZE, :] = grad_v.astype(jnp.bfloat16)
    half = heads * SIZE
    own = pl.multiple_of(core * half, half)
    w_kv = jnp.concatenate(
        [w_ref[pl.ds(width + own, half), :], w_ref[pl.ds(2 * width + own, half), :]], axis=0
    )
    kv = kvt[...].T
    for b in range(length // block):
        span = slice(b * block, (b + 1) * block)
        total = jnp.dot(
            (grad_q[b] * scale).astype(jnp.bfloat16), w_ref[:width, :], preferred_element_type=jnp.float32
        ) + jnp.dot(kv[span], w_kv, preferred_element_type=jnp.float32)
        rows = pair_ref.shape[0] // length
        first = pl.program_id(0) + b * block * rows
        pair_ref[pl.ds(first, block, stride=rows), :] = total


def run_grads(acts, bias, weight, name):
    rows, length, width = acts[0].shape
    heads = bias.shape[1]
    out = jax.ShapeDtypeStruct((length * rows, width), jnp.float32)
    swapped = pltpu.VMEM((width, length), jnp.bfloat16)
    return pl.pallas_call(
        grad_rows,
        grid=(rows,),
        in_specs=[per_row(x) for x in acts]
        + [whole(bias), whole(weight)],
        out_specs=whole(out),
        out_shape=out,
        scratch_shapes=[pltpu.VMEM((heads, length, length), jnp.float32)] + [swapped] * 3,
        compiler_params=pltpu.CompilerParams(dimension_semantics=("arbitrary",), vmem_limit_bytes=VMEM),
        cost_estimate=estimate(5, acts, heads),
        name=name,
    )(*acts, bias, weight)


def sum_groups(wire_ref, *out_refs):
    tall = wire_ref.shape[3]
    for m, out_ref in enumerate(out_refs):
        for c in range(wire_ref.shape[1]):
            total = wire_ref[0, c, m].astype(jnp.float32)
            for s in range(1, wire_ref.shape[0]):
                total += wire_ref[s, c, m].astype(jnp.float32)
            out_ref[c * tall : (c + 1) * tall, :] = total.astype(out_ref.dtype)


def finish(bias_ref, total_ref, *refs):
    *piece_refs, out_ref = refs
    total = total_ref[...]
    for ref in piece_refs:
        total += ref[...].astype(jnp.float32)
    heads, tall, _ = bias_ref.shape
    for h in range(heads):
        factor = jnp.exp(bias_ref[h].astype(jnp.float32))
        out_ref[h] = total[h * tall : (h + 1) * tall] * factor


def group_sum(wire):
    _, cores, lines, tall, length = wire.shape
    out = lambda kind: jax.ShapeDtypeStruct((cores * tall, length), kind)
    return pl.pallas_call(
        sum_groups,
        out_shape=[out(jnp.float32)] + [out(wire.dtype)] * (lines - 1),
        name="group_sum",
    )(wire)


def local(query_act, key_act, value_act, attn_out, grad_out, pair_bias, log_norm, back_weight):
    heads, tall, length = pair_bias.shape
    lines, cores = lax.axis_size(Z), lax.axis_size(C)
    groups = lax.axis_size((Z0, Y, X))
    near = heads // cores
    shape = (groups, cores, lines, near * tall, length)

    own = (query_act, key_act, value_act, attn_out, grad_out, log_norm)
    other = tuple(across(x) for x in own)

    line = jnp.stack([pair_bias] + [swapped_with(pair_bias, Z, m) for m in range(1, lines)], 1)
    line = line.reshape(1, cores, near, lines, tall, length).transpose(0, 1, 3, 2, 4, 5)
    line = line.reshape(1, cores, lines * near * tall, length)
    tiles = jnp.broadcast_to(line, (groups, *line.shape[1:])).reshape(groups * cores, -1, length)
    bias = exchange(tiles, NEAR).reshape(shape)

    terms = run_scores(other, shape, run_scores(own, shape))
    off_chip = tuple(pltpu.with_memory_space_constraint(x, pltpu.HBM) for x in other)
    sent = run_grads(off_chip, bias, back_weight, "partner_grads")
    kept = run_grads(own, bias, back_weight, "own_grads")

    pair_rows = (kept + across(sent)).astype(jnp.bfloat16)
    rows, _, width = query_act.shape
    devices = length // rows
    arrived = exchange(pair_rows.reshape(devices, rows * rows, width), ROWS)
    arrived = arrived.reshape(devices, rows, rows, width)
    column_grad = jnp.swapaxes(arrived, 0, 1).reshape(rows, length, width)

    wire = exchange(terms.reshape(groups * cores, -1, length), NEAR).reshape(shape)
    total, *pieces = group_sum(wire)
    pieces = [swapped_with(piece, Z, m) for m, piece in enumerate(pieces, 1)]
    column_grad, *pieces = lax.optimization_barrier((column_grad, *pieces))
    bias_grad = pl.pallas_call(
        finish, out_shape=jax.ShapeDtypeStruct(pair_bias.shape, jnp.float32), name="finish"
    )(pair_bias, total, *pieces)
    return (column_grad, bias_grad)


def solution(mesh):
    finer = Mesh(mesh.devices.reshape(4, 2, 2, 4, 2, mesh.shape["dp"]), (*ROWS, "dp"))
    row = P(DP_ROWS, None, None)
    return jax.shard_map(
        local,
        mesh=finer,
        in_specs=(row, row, row, row, row, P(None, DP_ROWS, None), row, P()),
        out_specs=(P(ROWS, "dp", None), P(None, DP_ROWS, None)),
        check_vma=False,
    )
```

```python
import functools

import jax
import jax.numpy as jnp
from jax import lax
from jax.experimental import pallas as pl
from jax.experimental.pallas import tpu as pltpu
from jax.sharding import Mesh
from jax.sharding import PartitionSpec as P

Z, Z0, Y, X, C = ("rows_0", "rows_1", "rows_2", "rows_3", "rows_4")
NEAR = (Z0, Y, X, C)
ROWS = (Z,) + NEAR
DP_ROWS = ("dp",) + ROWS
PLANE = (Y, X)
LINE = (Z, C)
SIZE = 32
VMEM = 20 * 1024 * 1024
LOG2E = 1.4426950408889634


def exchange(x, axes):
    return lax.all_to_all(x, axes, split_axis=0, concat_axis=0, tiled=True)


def swapped_with(x, axes, mask):
    n = lax.axis_size(axes)
    return lax.ppermute(x, axes, [(i, i ^ mask) for i in range(n)])


def across(x):
    return swapped_with(x, C, 1)


def placed(m, s, tall):
    groups = lax.axis_size((Z0, Y, X))
    return pl.ds(pl.multiple_of(((lax.axis_index(Z) ^ m) * groups + s) * tall, tall), tall)


def halves(lower, upper):
    cut = lower.shape[0] // 2
    first = jnp.concatenate([lower[:cut], upper[:cut]], 0)
    return first, jnp.concatenate([lower[cut:], upper[cut:]], 0)


def score_rows(first, q_ref, k_ref, v_ref, o_ref, g_ref, ln_ref, *rest):
    if first:
        (sum_ref,) = rest
    else:
        before_ref, wire_ref, sum_ref = rest
    step = pl.program_id(0)
    heads, length = sum_ref.shape[:2]
    width = q_ref.shape[2]
    core = lax.axis_index(C)

    @pl.when(step == 0)
    def _():
        sum_ref[...] = jnp.zeros_like(sum_ref) if first else before_ref[...]

    q, g = q_ref[0], g_ref[0]
    kt, vt = k_ref[0].T, v_ref[0].T
    product = g.astype(jnp.float32) * o_ref[0].astype(jnp.float32)
    lane = lax.broadcasted_iota(jnp.int32, (1, width), 1)
    ln_rows = ln_ref[0]
    ln_columns = jnp.concatenate([ln_rows, ln_rows], 0).T
    ln_lane = lax.broadcasted_iota(jnp.int32, (1, ln_columns.shape[1]), 1)
    block = 512
    for h in range(heads):
        head = core * heads + h
        mine = (lane // SIZE) == head
        ln = jnp.sum(jnp.where(ln_lane == head, ln_columns, 0.0), axis=1, keepdims=True) * LOG2E
        delta = jnp.sum(jnp.where(mine, product, 0.0), axis=1, keepdims=True)
        qh = jnp.where(mine, q, jnp.zeros_like(q))
        gh = jnp.where(mine, g, jnp.zeros_like(g))
        for b in range(length // block):
            span = slice(b * block, (b + 1) * block)
            s = jnp.dot(qh[span], kt, preferred_element_type=jnp.float32)
            d = jnp.dot(gh[span], vt, preferred_element_type=jnp.float32)
            e = jnp.exp2(s * (SIZE**-0.5 * LOG2E) - ln[span])
            sum_ref[h, span, :] += e * (d - delta[span])

    if not first:

        @pl.when(step == pl.num_programs(0) - 1)
        def _():
            groups, _, lines, tall, _ = wire_ref.shape
            for s in range(groups):
                for m in range(lines):
                    rows = placed(m, s, tall)
                    sides = halves(sum_ref[0, rows, :], sum_ref[1, rows, :])
                    for c, side in enumerate(sides):
                        wire_ref[s, c, m] = side.astype(wire_ref.dtype)


def whole(x):
    return pl.BlockSpec(x.shape, lambda i: (0,) * len(x.shape))


def per_row(x):
    return pl.BlockSpec((1,) + x.shape[1:], lambda i: (i,) + (0,) * (len(x.shape) - 1))


def estimate(products, acts, heads):
    rows, length, width = acts[0].shape
    return pl.CostEstimate(
        flops=2 * products * rows * heads * length * length * width,
        bytes_accessed=8 * 1024 * 1024,
        transcendentals=rows * heads * length * length,
    )


def run_scores(acts, shape, before=None):
    first = before is None
    rows, length, _ = acts[0].shape
    heads = shape[1]
    square = jax.ShapeDtypeStruct((heads, length, length), jnp.float32)
    args = [*acts]
    in_specs = [per_row(x) for x in acts]
    outs = []
    scratch = []
    if first:
        outs.append(square)
    else:
        args.append(before)
        in_specs.append(whole(before))
        outs.append(jax.ShapeDtypeStruct(shape, jnp.bfloat16))
        scratch.append(pltpu.VMEM(square.shape, jnp.float32))
    return pl.pallas_call(
        functools.partial(score_rows, first),
        grid=(rows,),
        in_specs=in_specs,
        out_specs=whole(outs[0]),
        out_shape=outs[0],
        scratch_shapes=scratch,
        compiler_params=pltpu.CompilerParams(dimension_semantics=("arbitrary",), vmem_limit_bytes=VMEM),
        cost_estimate=estimate(2, acts, heads),
        name="own_scores" if first else "partner_scores",
    )(*args)


def grad_rows(q_ref, k_ref, v_ref, o_ref, g_ref, ln_ref, bias_ref, w_ref, pair_ref, b2, kvt, qt, gt):
    groups, heads, lines, tall, length = bias_ref.shape
    width = q_ref.shape[2]
    scale = SIZE**-0.5
    core = lax.axis_index(C)

    @pl.when(pl.program_id(0) == 0)
    def _():
        for s in range(groups):
            for m in range(lines):
                sides = [bias_ref[s, c, m].astype(jnp.float32) for c in range(2)]
                for h, both in enumerate(halves(*sides)):
                    b2[h, placed(m, s, tall), :] = both * LOG2E

    q, k, g = q_ref[0], k_ref[0], g_ref[0]
    qt[...] = q.T
    gt[...] = g.T
    kt, vt = k.T, v_ref[0].T
    product = g.astype(jnp.float32) * o_ref[0].astype(jnp.float32)
    lane = lax.broadcasted_iota(jnp.int32, (1, width), 1)
    ln_rows = ln_ref[0]
    ln_columns = jnp.concatenate([ln_rows, ln_rows], 0).T
    ln_lane = lax.broadcasted_iota(jnp.int32, (1, ln_columns.shape[1]), 1)
    block = 512
    grad_q = [None] * (length // block)
    for h in range(heads):
        head = core * heads + h
        mine = (lane // SIZE) == head
        ln = jnp.sum(jnp.where(ln_lane == head, ln_columns, 0.0), axis=1, keepdims=True) * LOG2E
        delta = jnp.sum(jnp.where(mine, product, 0.0), axis=1, keepdims=True)
        qh = jnp.where(mine, q, jnp.zeros_like(q))
        gh = jnp.where(mine, g, jnp.zeros_like(g))
        kh = jnp.where(mine, k, jnp.zeros_like(k))
        rows = pl.ds(pl.multiple_of(head * SIZE, SIZE), SIZE)
        qth = qt[rows, :]
        gth = gt[rows, :]
        grad_k = grad_v = None
        for b in range(length // block):
            span = slice(b * block, (b + 1) * block)
            s = jnp.dot(qh[span], kt, preferred_element_type=jnp.float32)
            d = jnp.dot(gh[span], vt, preferred_element_type=jnp.float32)
            prob = jnp.exp2(s * (SIZE**-0.5 * LOG2E) + b2[h, span, :] - ln[span])
            p = prob.astype(jnp.bfloat16)
            ds = (prob * (d - delta[span])).astype(jnp.bfloat16)
            gv = jnp.dot(gth[:, span], p, preferred_element_type=jnp.float32)
            gk = jnp.dot(qth[:, span], ds, preferred_element_type=jnp.float32)
            gq = jnp.dot(ds, kh, preferred_element_type=jnp.float32)
            grad_k = gk if grad_k is None else grad_k + gk
            grad_v = gv if grad_v is None else grad_v + gv
            grad_q[b] = gq if grad_q[b] is None else grad_q[b] + gq
        kvt[h * SIZE : (h + 1) * SIZE, :] = (grad_k * scale).astype(jnp.bfloat16)
        kvt[(heads + h) * SIZE : (heads + h + 1) * SIZE, :] = grad_v.astype(jnp.bfloat16)
    half = heads * SIZE
    own = pl.multiple_of(core * half, half)
    w_kv = jnp.concatenate(
        [w_ref[pl.ds(width + own, half), :], w_ref[pl.ds(2 * width + own, half), :]], axis=0
    )
    kv = kvt[...].T
    for b in range(length // block):
        span = slice(b * block, (b + 1) * block)
        total = jnp.dot(
            (grad_q[b] * scale).astype(jnp.bfloat16), w_ref[:width, :], preferred_element_type=jnp.float32
        ) + jnp.dot(kv[span], w_kv, preferred_element_type=jnp.float32)
        rows = pair_ref.shape[0] // length
        first = pl.program_id(0) + b * block * rows
        pair_ref[pl.ds(first, block, stride=rows), :] = total


def run_grads(acts, bias, weight, name):
    rows, length, width = acts[0].shape
    heads = bias.shape[1]
    out = jax.ShapeDtypeStruct((length * rows, width), jnp.float32)
    swapped = pltpu.VMEM((width, length), jnp.bfloat16)
    return pl.pallas_call(
        grad_rows,
        grid=(rows,),
        in_specs=[per_row(x) for x in acts]
        + [whole(bias), whole(weight)],
        out_specs=whole(out),
        out_shape=out,
        scratch_shapes=[pltpu.VMEM((heads, length, length), jnp.float32)] + [swapped] * 3,
        compiler_params=pltpu.CompilerParams(dimension_semantics=("arbitrary",), vmem_limit_bytes=VMEM),
        cost_estimate=estimate(5, acts, heads),
        name=name,
    )(*acts, bias, weight)


def sum_groups(wire_ref, *out_refs):
    tall = wire_ref.shape[3]
    for m, out_ref in enumerate(out_refs):
        for c in range(wire_ref.shape[1]):
            total = wire_ref[0, c, m].astype(jnp.float32)
            for s in range(1, wire_ref.shape[0]):
                total += wire_ref[s, c, m].astype(jnp.float32)
            near = out_ref.shape[0] // wire_ref.shape[1]
            for h in range(near):
                part = total[h * tall // near : (h + 1) * tall // near]
                out_ref[c * near + h] = part.astype(out_ref.dtype)


def group_sum(wire, shape):
    lines = wire.shape[2]
    out = lambda kind: jax.ShapeDtypeStruct(shape, kind)
    return pl.pallas_call(
        sum_groups,
        out_shape=[out(jnp.float32)] + [out(wire.dtype)] * (lines - 1),
        name="group_sum",
    )(wire)


def local(query_act, key_act, value_act, attn_out, grad_out, pair_bias, log_norm, back_weight):
    heads, tall, length = pair_bias.shape
    lines, cores = lax.axis_size(Z), lax.axis_size(C)
    groups = lax.axis_size((Z0, Y, X))
    near = heads // cores
    shape = (groups, cores, lines, near * tall, length)

    own = (query_act, key_act, value_act, attn_out, grad_out, log_norm)
    other = tuple(across(x) for x in own)

    line = jnp.stack([pair_bias] + [swapped_with(pair_bias, Z, m) for m in range(1, lines)], 1)
    line = line.reshape(1, cores, near, lines, tall, length).transpose(0, 1, 3, 2, 4, 5)
    line = line.reshape(1, cores, lines * near * tall, length)
    tiles = jnp.broadcast_to(line, (groups, *line.shape[1:])).reshape(groups * cores, -1, length)
    bias = exchange(tiles, NEAR).reshape(shape)

    terms = run_scores(other, shape, run_scores(own, shape))
    off_chip = tuple(pltpu.with_memory_space_constraint(x, pltpu.HBM) for x in other)
    sent = run_grads(off_chip, bias, back_weight, "partner_grads")
    kept = run_grads(own, bias, back_weight, "own_grads")

    pair_rows = (kept + across(sent)).astype(jnp.bfloat16)
    rows, _, width = query_act.shape
    devices = length // rows
    arrived = exchange(pair_rows.reshape(devices, rows * rows, width), ROWS)
    arrived = arrived.reshape(devices, rows, rows, width)
    column_grad = jnp.swapaxes(arrived, 0, 1).reshape(rows, length, width)

    wire = exchange(terms.reshape(groups * cores, -1, length), NEAR).reshape(shape)
    total, *pieces = group_sum(wire, pair_bias.shape)
    for m, piece in enumerate(pieces, 1):
        total += swapped_with(piece, Z, m).astype(jnp.float32)
    bias_grad = total * jnp.exp(pair_bias.astype(jnp.float32))
    return (column_grad, bias_grad)


def solution(mesh):
    finer = Mesh(mesh.devices.reshape(4, 2, 2, 4, 2, mesh.shape["dp"]), (*ROWS, "dp"))
    row = P(DP_ROWS, None, None)
    return jax.shard_map(
        local,
        mesh=finer,
        in_specs=(row, row, row, row, row, P(None, DP_ROWS, None), row, P()),
        out_specs=(P(ROWS, "dp", None), P(None, DP_ROWS, None)),
        check_vma=False,
    )
```
